256 devices in a mesh: section: 2 (over core), dp: 16 (over z, x_lo), tensor: 8 (over y, x_hi).
Axes of the slice: x: 4 (x_hi: 2, x_lo: 2; x = x_hi * 2 + x_lo), y: 4, z: 8, core: 2. Of those that a mesh axis runs over, the one named last changes fastest.
Arguments:
- tokens: bfloat16 [2048, 4096], P('dp', 'tensor'), may hold values from -6 to 6
- gain: bfloat16 [2, 4096], P('section', 'tensor'), may hold values from 0.099609375 to 1.8984375
- w_up: bfloat16 [2, 4096, 5120], P('section', 'dp', 'tensor'), may hold values from -0.09375 to 0.09375
- w_down: bfloat16 [2, 5120, 4096], P('section', 'tensor', 'dp'), may hold values from -0.078125 to 0.078125
- cotangent: bfloat16 [2, 2048, 4096], P('section', 'dp'), may hold values from -6 to 6
Outputs:
- states: bfloat16 [2, 2048, 4096], P('section', 'dp', 'tensor')
- grad_down: bfloat16 [2, 5120, 4096], P('section', 'tensor', 'dp')
The draws below stay inside these ranges and needn't reach their ends.
All inputs are finite; a program needn't handle non-finite values.
Results may differ from the reference program's by a relative error of at most 0.02.
Values may be sent and summed in bfloat16 or wider, within the bound.
A program may use at most 64 MiB of HBM per device.

```python
import jax
import jax.numpy as jnp
from jax import lax

WIDTH = 4096
HIDDEN_SIZE = 5120
TOK_DEV = 128
TOKENS = 2048
LAYERS = 2
N_SECTION = 2
N_DP = 16
N_TENSOR = 8


def block_levels(own_key, dims, pieces, low, high):
    level = 1.0
    for dim, blocks in pieces:
        steps = jax.random.uniform(jax.random.fold_in(jax.random.fold_in(own_key, 6), dim), (blocks,), jnp.float32, low / len(pieces), high / len(pieces))
        level = level * jnp.repeat(jnp.exp(steps), dims[dim] // blocks).reshape((-1,) + (1,) * (len(dims) - 1 - dim))
    return level


def normal_values(key, extent, deviation, bound, cuts=(), dtype=jnp.bfloat16):
    drawn = deviation * jax.random.normal(key, extent, jnp.float32)
    if cuts:
        drawn = drawn * block_levels(key, extent, cuts, -0.22, 0.18)
    return jnp.clip(drawn, -bound, bound).astype(dtype)


def setup_inputs(seed: int = 0) -> dict:
    arg_keys = jax.random.split(jax.random.key(seed), 6)
    return {
        "tokens": normal_values(arg_keys[0], (TOKENS, WIDTH), 1.0, 6.0, ((0, 16), (1, 8))),
        "gain": jnp.clip(1.0 + 0.18 * jax.random.normal(arg_keys[1], (LAYERS, WIDTH), jnp.float32), 0.099609375, 1.8984375).astype(jnp.bfloat16),
        "w_up": normal_values(arg_keys[2], (LAYERS, WIDTH, HIDDEN_SIZE), WIDTH ** -0.5, 0.09375, ((0, 2), (1, 16), (2, 8))),
        "w_down": normal_values(arg_keys[3], (LAYERS, HIDDEN_SIZE, WIDTH), HIDDEN_SIZE ** -0.5, 0.078125, ((0, 2), (1, 8), (2, 16))),
        "cotangent": normal_values(arg_keys[4], (LAYERS, TOKENS, WIDTH), 1.0, 6.0, ((0, 2), (1, 16))),
    }


EPS = 1e-06

def layer_ref(acts, gain_row, up_mat, down_mat):
    acts_f = acts.astype(jnp.float32)
    mean_sq = lax.optimization_barrier(jnp.mean(acts_f * acts_f, axis=1, keepdims=True))
    normed = (acts_f * lax.rsqrt(mean_sq + EPS) * gain_row.astype(jnp.float32)).astype(jnp.bfloat16)
    pre_act = jnp.dot(normed, up_mat, preferred_element_type=jnp.float32)
    hidden = jax.nn.gelu(pre_act, approximate=True).astype(jnp.bfloat16)
    group_width = HIDDEN_SIZE // N_TENSOR
    summed = jnp.zeros(acts.shape, jnp.float32)
    for group_id in range(N_TENSOR):
        lower = group_id * group_width
        partial_value = jnp.dot(hidden[:, lower:lower + group_width], down_mat[lower:lower + group_width, :], preferred_element_type=jnp.float32).astype(jnp.bfloat16)
        summed = summed + lax.optimization_barrier(partial_value).astype(jnp.float32)
    return ((acts_f + summed).astype(jnp.bfloat16), hidden)

def reference(tokens, gain, w_up, w_down, cotangent):
    acts = tokens
    states = []
    grads = []
    for layer_id in range(N_SECTION):
        acts, hidden = layer_ref(acts, gain[layer_id], w_up[layer_id], w_down[layer_id])
        states.append(acts)
        grad_sum = jnp.zeros((HIDDEN_SIZE, WIDTH), jnp.float32)
        for peer_id in range(N_DP):
            lower = peer_id * TOK_DEV
            partial_value = lax.dot_general(hidden[lower:lower + TOK_DEV], cotangent[layer_id][lower:lower + TOK_DEV], (((0,), (0,)), ((), ())), preferred_element_type=jnp.float32).astype(jnp.bfloat16)
            grad_sum = grad_sum + lax.optimization_barrier(partial_value).astype(jnp.float32)
        grads.append(grad_sum.astype(jnp.bfloat16))
    return (jnp.stack(states), jnp.stack(grads))
```

```python
import jax
import jax.numpy as jnp
from jax import lax
from jax.experimental import pallas as pl
from jax.experimental.pallas import tpu as pltpu
from jax.sharding import Mesh
from jax.sharding import PartitionSpec as P

NZ, NA, NY, NB = 8, 2, 4, 2
NT = NY * NB
NP = NA * NT
EPS = 1e-06
MESH = pl.DeviceIdType.MESH
F32 = jnp.float32
BF16 = jnp.bfloat16
OFFSETS = [(da, dy, db) for da in range(NA) for dy in range(NY) for db in range(NB)]
NT_DIMS = (((1,), (1,)), ((), ()))


def remote(src, dst, send, recv, **where):
    return pltpu.make_async_remote_copy(
        src_ref=src, dst_ref=dst, send_sem=send, recv_sem=recv, device_id=where, device_id_type=MESH
    )


def ring_parts(buf, z, right_send, right_recv, left_send, left_recv):
    rows = buf.shape[1] // 2

    def part(origin, half):
        return buf.at[origin, pl.ds(half * rows, rows), :]

    def right(r):
        half = r % 2
        piece = part(lax.rem(z + NZ - r // 2, NZ), half)
        return remote(piece, piece, right_send.at[r], right_recv.at[r], z=lax.rem(z + 1, NZ))

    def left(r):
        half = 1 if r == 6 else r % 2
        piece = part(lax.rem(z + r // 2, NZ), half)
        return remote(piece, piece, left_send.at[r], left_recv.at[r], z=lax.rem(z + NZ - 1, NZ))

    def from_left(r):
        piece = part(lax.rem(z + 2 * NZ - 1 - r // 2, NZ), r % 2)
        return remote(piece, piece, right_send.at[r], right_recv.at[r], z=lax.rem(z + 1, NZ))

    def from_right(r):
        half = 1 if r == 6 else r % 2
        piece = part(lax.rem(z + 1 + r // 2, NZ), half)
        return remote(piece, piece, left_send.at[r], left_recv.at[r], z=lax.rem(z + NZ - 1, NZ))

    return right, left, from_left, from_right


def ring_start(ring):
    right, left, _, _ = ring
    for r in (0, 1):
        right(r).start()
        left(r).start()


def ring_arrive(ring, r):
    right, left, from_left, from_right = ring
    from_left(r).wait_recv()
    if r + 2 <= 6:
        if r != 5:
            right(r + 2).start()
    from_right(r).wait_recv()
    if r in (0, 1, 2, 3):
        left(r + 2).start()
    if r == 5:
        left(6).start()


def ring_drain(ring):
    right, left, _, _ = ring
    for r in range(7):
        right(r).wait_send()
        left(r).wait_send()


def kernel(
    tokens, gain, up_t, down, cot, states, grad,
    up_all, down_all, x_all, h_all, h_own, c_z, c_all, gain_all, part_send, part_recv,
    x_own, result, acc_h, acc_g, g_send, g_recv,
    ex_send, ex_recv, own_sem, gain_send, gain_recv, x_send, x_recv, p_send, p_recv,
    cz_send, cz_recv, ca_send, ca_recv, next_send, next_recv, g_ssem, g_rsem,
    rs0, rr0, ls0, lr0, rs1, rr1, ls1, lr1, rs2, rr2, ls2, lr2, gate,
):
    s = lax.axis_index("section")
    z = lax.axis_index("z")
    a = lax.axis_index("a")
    y = lax.axis_index("y")
    b = lax.axis_index("b")
    t = y * NB + b
    first = s == 0
    second = s == 1
    half = up_t.shape[0] // 2
    cols = up_t.shape[1]
    rows = tokens.shape[0]
    slab = tokens.shape[1]
    sub = rows // NT
    other_a = 1 - a

    def peer(o):
        da, dy, db = OFFSETS[o]
        return {"a": lax.rem(a + da, NA), "y": lax.rem(y + dy, NY), "b": lax.rem(b + db, NB)}

    def source(o):
        da, dy, db = OFFSETS[o]
        return (
            lax.rem(a + da, NA),
            lax.rem(y + NY - dy, NY),
            lax.rem(b + db, NB),
        )

    @pl.when(first)
    def _():
        pltpu.make_async_copy(tokens, x_own, own_sem.at[4]).start()

    my_rows = pl.ds(pl.multiple_of(half * a, half), half)
    my_cols = pl.ds(pl.multiple_of(cols * a, cols), cols)
    own_up = pltpu.make_async_copy(up_t.at[my_rows, :], up_all.at[z, :, my_cols], own_sem.at[0])
    own_down = pltpu.make_async_copy(down.at[my_rows, :], down_all.at[z, :, my_cols], own_sem.at[1])
    own_gain = pltpu.make_async_copy(gain, gain_all.at[t], own_sem.at[2])
    cot_rows = pl.ds(pl.multiple_of(sub * t, sub), sub)

    def cot_cols(index):
        return pl.ds(pl.multiple_of(slab * index, slab), slab)

    own_cot = pltpu.make_async_copy(cot.at[cot_rows, cot_cols(z)], c_z.at[z], own_sem.at[3])
    own_up.start()
    own_down.start()
    own_gain.start()
    own_cot.start()

    barrier = pltpu.get_barrier_semaphore()
    for dz in range(1, NZ):
        pl.semaphore_signal(barrier, inc=1, device_id={"z": lax.rem(z + dz, NZ)}, device_id_type=MESH)
    for o in range(1, NP):
        pl.semaphore_signal(barrier, inc=1, device_id=peer(o), device_id_type=MESH)
    pl.semaphore_signal(barrier, inc=1, device_id={"section": 1 - s}, device_id_type=MESH)
    pl.semaphore_wait(barrier, NZ - 1 + NP - 1 + 1)

    their_rows = pl.ds(pl.multiple_of(half * other_a, half), half)
    ex_up = remote(up_t.at[their_rows, :], up_all.at[z, :, my_cols], ex_send.at[0], ex_recv.at[0], a=other_a)
    ex_down = remote(down.at[their_rows, :], down_all.at[z, :, my_cols], ex_send.at[1], ex_recv.at[1], a=other_a)
    ex_up.start()

    def gain_copy(o):
        return remote(gain, gain_all.at[t], gain_send.at[o], gain_recv.at[o], **peer(o))

    for o in range(1, NT):
        gain_copy(o).start()

    x_slot = x_all.at[t, pl.ds(pl.multiple_of(rows * a, rows), rows), :]
    x_mine = pltpu.make_async_copy(x_own, x_slot, own_sem.at[5])

    def x_copy(o):
        return remote(x_own, x_slot, x_send.at[o], x_recv.at[o], **peer(o))

    def x_start():
        x_mine.start()
        for o in range(1, NP):
            x_copy(o).start()

    def x_wait():
        x_mine.wait()
        for o in range(1, NP):
            sa, sy, sb = source(o)
            slot = x_all.at[sy * NB + sb, pl.ds(pl.multiple_of(rows * sa, rows), rows), :]
            remote(x_own, slot, x_send.at[o], x_recv.at[o], **peer(o)).wait_recv()
        for o in range(1, NT):
            sa, sy, sb = source(o)
            remote(gain, gain_all.at[sy * NB + sb], gain_send.at[o], gain_recv.at[o], **peer(o)).wait_recv()

    @pl.when(first)
    def _():
        pltpu.make_async_copy(tokens, x_own, own_sem.at[4]).wait()
        x_start()

    ex_down.start()

    def cz_copy(dz):
        to = lax.rem(z + dz, NZ)
        return remote(cot.at[cot_rows, cot_cols(to)], c_z.at[z], cz_send.at[dz], cz_recv.at[dz], z=to)

    def cz_start():
        for dz in range(1, NZ):
            cz_copy(dz).start()

    place = a * NT + t
    c_mine = pltpu.make_async_copy(c_z, c_all.at[place], own_sem.at[6])

    def ca_copy(o):
        return remote(c_z, c_all.at[place], ca_send.at[o], ca_recv.at[o], **peer(o))

    def ca_start():
        own_cot.wait()
        for dz in range(1, NZ):
            slot = c_z.at[lax.rem(z + NZ - dz, NZ)]
            remote(slot, slot, cz_send.at[dz], cz_recv.at[dz], z=lax.rem(z + dz, NZ)).wait_recv()
        c_mine.start()
        for o in range(1, NP):
            ca_copy(o).start()

    def ca_wait():
        c_mine.wait()
        for o in range(1, NP):
            sa, sy, sb = source(o)
            remote(c_z, c_all.at[sa * NT + sy * NB + sb], ca_send.at[o], ca_recv.at[o], **peer(o)).wait_recv()

    @pl.when(second)
    def _():
        cz_start()
        ca_start()

    own_gain.wait()
    own_up.wait()
    own_down.wait()

    up_ring = ring_parts(up_all, z, rs0, rr0, ls0, lr0)
    down_ring = ring_parts(down_all, z, rs1, rr1, ls1, lr1)
    h_ring = ring_parts(h_all, z, rs2, rr2, ls2, lr2)

    ex_up.wait_recv()

    @pl.when(second)
    def _():
        pl.semaphore_wait(gate, 1)

    ring_start(up_ring)
    for r in range(7):
        ring_arrive(up_ring, r)
    ex_down.wait_recv()
    ring_start(down_ring)

    def up_product():
        acc_h[...] = jnp.zeros_like(acc_h)

        def step(index, squares):
            block = x_all[index].astype(F32)
            squares = squares + jnp.sum(block * block, axis=1, keepdims=True)
            scaled = (block * gain_all[index]).astype(BF16)
            acc_h[...] += lax.dot_general(scaled, up_all[index], NT_DIMS, preferred_element_type=F32)
            return squares

        squares = lax.fori_loop(0, NT, step, jnp.zeros((NA * rows, 1), F32))
        inverse_rms = lax.rsqrt(squares * (1.0 / (NT * slab)) + EPS)
        hidden = jax.nn.gelu(acc_h[...] * inverse_rms, approximate=True).astype(BF16)
        h_own[...] = hidden
        h_all[z] = hidden.T

    def part_copy(index, to_a):
        to_y, to_b = index // NB, lax.rem(index, NB)
        offset = (
            lax.rem(to_a + NA - a, NA) * NT
            + lax.rem(to_y + NY - y, NY) * NB
            + lax.rem(to_b + NB - b, NB)
        )
        piece = part_send.at[index, pl.ds(to_a * rows, rows), :]
        copy = remote(
            piece, part_recv.at[offset], p_send.at[offset], p_recv.at[offset], a=to_a, y=to_y, b=to_b
        )
        return offset, copy

    def down_product(index):
        part_send[index] = lax.dot_general(
            h_own[...], down_all[index], (((1,), (0,)), ((), ())), preferred_element_type=F32
        ).astype(BF16)
        for to_a in range(NA):
            offset, copy = part_copy(index, to_a)

            @pl.when(offset != 0)
            def _():
                copy.start()

    @pl.when(first)
    def _():
        x_wait()
        up_product()
        for r in range(7):
            ring_arrive(down_ring, r)
            if r == 0:
                down_product(z)
            if r in (1, 3, 5):
                down_product(lax.rem(z + NZ - 1 - r // 2, NZ))
                down_product(lax.rem(z + 1 + r // 2, NZ))
        down_product(lax.rem(z + 4, NZ))
        pl.semaphore_signal(gate, inc=1, device_id={"section": 1 - s}, device_id_type=MESH)

    @pl.when(second)
    def _():
        for r in range(7):
            ring_arrive(down_ring, r)
        remote(result, x_own, next_send, next_recv, section=1 - s).wait_recv()
        x_start()
        x_wait()
        up_product()

        @pl.loop(0, NZ)
        def _(k):
            down_product(lax.rem(z + k, NZ))

    def finish_states():
        mine = part_send[t, pl.ds(pl.multiple_of(rows * a, rows), rows), :]
        for o in range(1, NP):
            pltpu.make_async_copy(part_recv.at[o], part_recv.at[o], p_recv.at[o]).wait()

        def add(o, total):
            return total + part_recv[o].astype(F32)

        total = lax.fori_loop(1, NP, add, x_own[...].astype(F32) + mine.astype(F32))
        result[...] = total.astype(BF16)
        states[...] = result[...]

    hand_on = remote(result, x_own, next_send, next_recv, section=1 - s)

    @pl.when(first)
    def _():
        finish_states()
        hand_on.start()
        cz_start()
        ring_start(h_ring)
        ca_start()
        for r in range(7):
            ring_arrive(h_ring, r)

    @pl.when(second)
    def _():
        ring_start(h_ring)
        for r in range(7):
            ring_arrive(h_ring, r)
        finish_states()

    ca_wait()
    acc_g[...] = jnp.zeros_like(acc_g)

    @pl.loop(0, NZ)
    def _(index):
        block = c_all[:, pl.ds(index, 1)].reshape(NP * sub, slab)
        acc_g[...] += jnp.dot(h_all[index], block, preferred_element_type=F32)

    g_send[...] = acc_g[...].astype(BF16)
    their_cols = pl.ds(pl.multiple_of(cols * other_a, cols), cols)
    swap = remote(g_send.at[:, their_cols], g_recv, g_ssem, g_rsem, a=other_a)
    swap.start()
    grad[my_rows, :] = g_send[:, my_cols]
    swap.wait_recv()
    grad[their_rows, :] = g_recv[...]

    swap.wait_send()
    ex_up.wait_send()
    ex_down.wait_send()
    for o in range(1, NT):
        gain_copy(o).wait_send()
    for o in range(1, NP):
        x_copy(o).wait_send()
        ca_copy(o).wait_send()
        pltpu.make_async_copy(part_recv.at[o], part_recv.at[o], p_send.at[o]).wait()
    for dz in range(1, NZ):
        cz_copy(dz).wait_send()

    @pl.when(first)
    def _():
        hand_on.wait_send()

    ring_drain(up_ring)
    ring_drain(down_ring)
    ring_drain(h_ring)


def body(tokens, gain, w_up, w_down, cotangent):
    rows, slab = tokens.shape
    cols, hidden = w_up.shape[1:]
    half = hidden // 2
    dma = pltpu.SemaphoreType.DMA
    vmem = pl.BlockSpec(memory_space=pltpu.VMEM)
    states, grad = pl.pallas_call(
        kernel,
        out_shape=(
            jax.ShapeDtypeStruct((rows, slab), BF16),
            jax.ShapeDtypeStruct((hidden, cols), BF16),
        ),
        in_specs=[vmem] * 5,
        out_specs=(vmem, vmem),
        scratch_shapes=[
            pltpu.VMEM((NZ, half, NA * cols), BF16),
            pltpu.VMEM((NZ, half, NA * cols), BF16),
            pltpu.VMEM((NT, NA * rows, slab), BF16),
            pltpu.VMEM((NZ, half, NA * rows), BF16),
            pltpu.VMEM((NA * rows, half), BF16),
            pltpu.VMEM((NZ, rows // NT, slab), BF16),
            pltpu.VMEM((NP, NZ, rows // NT, slab), BF16),
            pltpu.VMEM((NT, 1, slab), F32),
            pltpu.VMEM((NZ, NA * rows, slab), BF16),
            pltpu.VMEM((NP, rows, slab), BF16),
            pltpu.VMEM((rows, slab), BF16),
            pltpu.VMEM((rows, slab), BF16),
            pltpu.VMEM((NA * rows, half), F32),
            pltpu.VMEM((half, NA * cols), F32),
            pltpu.VMEM((half, NA * cols), BF16),
            pltpu.VMEM((half, cols), BF16),
            dma((2,)), dma((2,)), dma((7,)), dma((NT,)), dma((NT,)), dma((NP,)), dma((NP,)), dma((NP,)), dma((NP,)),
            dma((NZ,)), dma((NZ,)), dma((NP,)), dma((NP,)), dma, dma, dma, dma,
        ]
        + [dma((7,))] * 12
        + [pltpu.SemaphoreType.REGULAR],
        compiler_params=pltpu.CompilerParams(
            collective_id=0, has_side_effects=True, vmem_limit_bytes=48 * 1024 * 1024
        ),
    )(tokens, gain.astype(F32), w_up[0].T, w_down[0], cotangent[0])
    return states[None], grad[None]


def solution(mesh):
    torus = Mesh(
        mesh.devices.reshape(mesh.shape["section"], NZ, NA, NY, NB), ("section", "z", "a", "y", "b")
    )
    dp, tensor = ("z", "a"), ("y", "b")
    in_specs = (
        P(dp, tensor),
        P("section", tensor),
        P("section", dp, tensor),
        P("section", tensor, dp),
        P("section", dp, None),
    )
    out_specs = (P("section", dp, tensor), P("section", tensor, dp))
    return jax.shard_map(body, mesh=torus, in_specs=in_specs, out_specs=out_specs, check_vma=False)
```

```python
import jax
import jax.numpy as jnp
from jax import lax
from jax.experimental import pallas as pl
from jax.experimental.pallas import tpu as pltpu
from jax.sharding import Mesh
from jax.sharding import PartitionSpec as P

NZ, NA, NY, NB = 8, 2, 4, 2
NT = NY * NB
NP = NA * NT
STEPS = NZ // 2 + 1
EPS = 1e-06
MESH = pl.DeviceIdType.MESH
F32 = jnp.float32
BF16 = jnp.bfloat16
OFFSETS = [(da, dy, db) for da in range(NA) for dy in range(NY) for db in range(NB)]
X_OFFSETS = [(1, 0, 0), (0, 0, 1), (1, 0, 1)]
Y_OFFSETS = [(0, dy, 0) for dy in range(1, NY)]
ROW_ROW = (((1,), (1,)), ((), ()))
COL_COL = (((0,), (0,)), ((), ()))


def remote(src, dst, send, recv, **where):
    return pltpu.make_async_remote_copy(
        src_ref=src, dst_ref=dst, send_sem=send, recv_sem=recv, device_id=where, device_id_type=MESH
    )


class Ring:
    def __init__(self, z, cut, piece, sems):
        self.z, self.cut, self.piece = z, cut, piece
        self.right_send, self.right_recv, self.left_send, self.left_recv = sems
        self.count = 7 * cut // 2

    def _copy(self, origin, q, to_right, r):
        piece = self.piece(lax.rem(origin, NZ), q)
        if to_right:
            return remote(piece, piece, self.right_send.at[r], self.right_recv.at[r], z=lax.rem(self.z + 1, NZ))
        return remote(piece, piece, self.left_send.at[r], self.left_recv.at[r], z=lax.rem(self.z + NZ - 1, NZ))

    def _left_q(self, r):
        return r % self.cut + (self.cut // 2 if r // self.cut == 3 else 0)

    def right(self, r):
        return self._copy(self.z + NZ - r // self.cut, r % self.cut, True, r)

    def left(self, r):
        return self._copy(self.z + r // self.cut, self._left_q(r), False, r)

    def start(self, r):
        self.right(r).start()
        self.left(r).start()

    def arrive(self, r):
        self._copy(self.z + 2 * NZ - 1 - r // self.cut, r % self.cut, True, r).wait_recv()
        if r + self.cut < self.count:
            self.right(r + self.cut).start()
        self._copy(self.z + 1 + r // self.cut, self._left_q(r), False, r).wait_recv()
        if r < 2 * self.cut:
            self.left(r + self.cut).start()
        elif 5 * self.cut // 2 <= r < 3 * self.cut:
            self.left(r + self.cut // 2).start()

    def arrive_step(self, k):
        for r in range(self.cut * (k - 1), min(self.cut * k, self.count)):
            self.arrive(r)

    def drain(self):
        for r in range(self.count):
            self.right(r).wait_send()
            self.left(r).wait_send()


class Plane:
    def __init__(self, me, own, slot, sems):
        self.me, self.own, self.slot = me, own, slot
        self.send1, self.recv1, self.send2, self.recv2 = sems

    def _at(self, *offsets):
        a, y, b = self.me
        for da, dy, db in offsets:
            a, y, b = lax.rem(a + NA - da, NA), lax.rem(y + NY - dy, NY), lax.rem(b + NB - db, NB)
        return a, y, b

    def _peer(self, offset):
        a, y, b = self.me
        da, dy, db = offset
        return {"a": lax.rem(a + da, NA), "y": lax.rem(y + dy, NY), "b": lax.rem(b + db, NB)}

    def _first(self, half, i, origin):
        offset = (X_OFFSETS, Y_OFFSETS)[half][i]
        n = 3 * half + i
        return remote(self.own(half), self.slot(origin, half), self.send1.at[n], self.recv1.at[n], **self._peer(offset))

    def _second(self, half, source, i, piece, origin):
        offset = (Y_OFFSETS, X_OFFSETS)[half][i]
        n = 12 * half + 3 * source + i
        return remote(piece, self.slot(origin, half), self.send2.at[n], self.recv2.at[n], **self._peer(offset))

    def start(self):
        for half in (0, 1):
            for i in range(3):
                self._first(half, i, self.me).start()
        for half in (0, 1):
            for i in range(3):
                self._second(half, 0, i, self.own(half), self.me).start()

    def relay(self):
        for i in range(3):
            for half in (0, 1):
                origin = self._at((X_OFFSETS, Y_OFFSETS)[half][i])
                self._first(half, i, origin).wait_recv()
                piece = self.slot(origin, half)
                for n in range(3):
                    self._second(half, i + 1, n, piece, origin).start()

    def wait(self):
        for half in (0, 1):
            for source in range(4):
                for i in range(3):
                    hops = [(Y_OFFSETS, X_OFFSETS)[half][i]]
                    if source:
                        hops.append((X_OFFSETS, Y_OFFSETS)[half][source - 1])
                    origin = self._at(*hops)
                    self._second(half, source, i, self.own(half), origin).wait_recv()

    def drain(self):
        for half in (0, 1):
            for i in range(3):
                self._first(half, i, self.me).wait_send()
            for source in range(4):
                for i in range(3):
                    self._second(half, source, i, self.own(half), self.me).wait_send()


def kernel(
    tokens, gain, up_t, down, cot, states, grad,
    up_all, down_all, x_all, x1_all, h_all, h_own, c_z, c_all, gain_all, part_send, part_recv, sums, final,
    acc_h, acc_g, g_send, g_recv,
    ex_send, ex_recv, own_sem, gain_send, gain_recv, rs_send, rs_recv, ag_send, ag_recv, f_send, f_recv,
    cz_send, cz_recv, back_send, back_recv, g_ssem, g_rsem,
    u0, u1, u2, u3, d0, d1, d2, d3, h0, h1, h2, h3, x0, x1, x2, x3, c0, c1, c2, c3, gate,
):
    s = lax.axis_index("section")
    z = lax.axis_index("z")
    a = lax.axis_index("a")
    y = lax.axis_index("y")
    b = lax.axis_index("b")
    t = y * NB + b
    place = a * NT + t
    me = (a, y, b)
    first = s == 0
    second = s == 1
    half = up_t.shape[0] // 2
    cols = up_t.shape[1]
    rows, slab = tokens.shape
    sub = rows // NT
    other_a = 1 - a

    def peer(o):
        da, dy, db = OFFSETS[o]
        return {"a": lax.rem(a + da, NA), "y": lax.rem(y + dy, NY), "b": lax.rem(b + db, NB)}

    def source(o):
        da, dy, db = OFFSETS[o]
        return lax.rem(a + NA - da, NA), lax.rem(y + NY - dy, NY), lax.rem(b + NB - db, NB)

    my_rows = pl.ds(pl.multiple_of(half * a, half), half)
    their_rows = pl.ds(pl.multiple_of(half * other_a, half), half)
    my_cols = pl.ds(pl.multiple_of(cols * a, cols), cols)
    their_cols = pl.ds(pl.multiple_of(cols * other_a, cols), cols)
    cot_rows = pl.ds(pl.multiple_of(sub * t, sub), sub)

    def cot_cols(index):
        return pl.ds(pl.multiple_of(slab * index, slab), slab)

    def c_slot(index):
        return c_z.at[index // 4, lax.rem(index, 4)]

    own_up = pltpu.make_async_copy(up_t.at[my_rows, :], up_all.at[z, a], own_sem.at[0])
    own_down = pltpu.make_async_copy(down.at[my_rows, :], down_all.at[z, a], own_sem.at[1])
    own_gain = pltpu.make_async_copy(gain, gain_all.at[t], own_sem.at[2])
    own_cot = pltpu.make_async_copy(cot.at[cot_rows, cot_cols(z)], c_slot(z), own_sem.at[3])
    own_x = [
        pltpu.make_async_copy(tokens.at[pl.ds(rows // 2 * i, rows // 2), :], x_all.at[a, t, i], own_sem.at[4 + i])
        for i in (0, 1)
    ]
    own_c = pltpu.make_async_copy(c_z, c_all.at[place], own_sem.at[6])
    own_up.start()
    own_down.start()
    own_gain.start()
    own_cot.start()

    @pl.when(first)
    def _():
        own_x[0].start()
        own_x[1].start()

    barrier = pltpu.get_barrier_semaphore()
    for dz in range(1, NZ):
        pl.semaphore_signal(barrier, inc=1, device_id={"z": lax.rem(z + dz, NZ)}, device_id_type=MESH)
    for o in range(1, NP):
        pl.semaphore_signal(barrier, inc=1, device_id=peer(o), device_id_type=MESH)
    for o in range(NP):
        pl.semaphore_signal(barrier, inc=1, device_id=dict(peer(o), section=1 - s), device_id_type=MESH)
    own_up.wait()
    pl.semaphore_wait(barrier, NZ - 1 + NP - 1 + NP)

    ex_up = remote(up_t.at[their_rows, :], up_all.at[z, a], ex_send.at[0], ex_recv.at[0], a=other_a)
    ex_down = remote(down.at[their_rows, :], down_all.at[z, a], ex_send.at[1], ex_recv.at[1], a=other_a)
    from_up = remote(up_t.at[their_rows, :], up_all.at[z, other_a], ex_send.at[0], ex_recv.at[0], a=other_a)
    from_down = remote(down.at[their_rows, :], down_all.at[z, other_a], ex_send.at[1], ex_recv.at[1], a=other_a)
    ex_up.start()

    quarter_rows = half // 2

    def quarter(buffer):
        def piece(origin, q):
            which = a if q < 2 else other_a
            return buffer.at[origin, which, pl.ds(q % 2 * quarter_rows, quarter_rows), :]

        return piece

    up_ring = Ring(z, 4, quarter(up_all), (u0, u1, u2, u3))
    down_ring = Ring(z, 4, quarter(down_all), (d0, d1, d2, d3))
    h_ring = Ring(z, 2, lambda origin, q: h_all.at[origin, pl.ds(q * quarter_rows, quarter_rows), :], (h0, h1, h2, h3))
    x_plane = Plane(
        me,
        lambda i: tokens.at[pl.ds(rows // 2 * i, rows // 2), :],
        lambda at, i: x_all.at[at[0], at[1] * NB + at[2], i],
        (x0, x1, x2, x3),
    )
    c_plane = Plane(
        me, lambda i: c_z.at[i], lambda at, i: c_all.at[at[0] * NT + at[1] * NB + at[2], i], (c0, c1, c2, c3)
    )

    def gain_copy(o):
        return remote(gain, gain_all.at[t], gain_send.at[o], gain_recv.at[o], **peer(o))

    def cz_copy(dz):
        to = lax.rem(z + dz, NZ)
        return remote(cot.at[cot_rows, cot_cols(to)], c_slot(z), cz_send.at[dz], cz_recv.at[dz], z=to)

    def cz_start():
        for dz in range(1, NZ):
            cz_copy(dz).start()

    def cz_wait():
        own_cot.wait()
        for dz in range(1, NZ):
            slot = c_slot(lax.rem(z + NZ - dz, NZ))
            remote(slot, slot, cz_send.at[dz], cz_recv.at[dz], z=lax.rem(z + dz, NZ)).wait_recv()

    def width(k):
        return 2 if 0 < k < NZ // 2 else 1

    def slot_of(k, j):
        return lax.rem(z + (k if j else NZ - k), NZ)

    def view(buffer, k, *index):
        return buffer.at[(k, *index)] if width(k) == 2 else buffer.at[(k, *index, 0)]

    def rs_copy(k, o):
        to = peer(o)
        there = to["a"] * NT + to["y"] * NB + to["b"]
        n = k * NP + o
        return remote(view(part_send, k, there), view(part_recv, k, o), rs_send.at[n], rs_recv.at[n], **to)

    def rs_start(k):
        for o in range(1, NP):
            rs_copy(k, o).start()

    def rs_sum(k, extra):
        for o in range(1, NP):
            rs_copy(k, o).wait_recv()
        for j in range(width(k)):
            total = part_send[k, place, j].astype(F32)
            if extra is not None:
                total = total + extra(slot_of(k, j))
            for o in range(1, NP):
                total = total + part_recv[k, o, j].astype(F32)
            sums[k, j] = total.astype(BF16)

    def ag_copy(k, o):
        n = k * NP + o
        return remote(view(sums, k), view(x1_all, k, place), ag_send.at[n], ag_recv.at[n], section=1, **peer(o))

    def ag_start(k):
        for o in range(NP):
            ag_copy(k, o).start()

    def ag_wait(k):
        for o in range(NP):
            sa, sy, sb = source(o)
            n = k * NP + o
            slot = view(x1_all, k, sa * NT + sy * NB + sb)
            remote(view(sums, k), slot, ag_send.at[n], ag_recv.at[n], section=0, **peer(o)).wait_recv()

    def store_part(k, j, which, product):
        part_send[k, :, j, :, pl.ds(which * cols, cols)] = product.astype(BF16).reshape(NP, sub, cols)

    def down_first(k, j):
        for which in range(NA):
            weights = down_all[slot_of(k, j), which]
            store_part(k, j, which, jnp.dot(h_own[...], weights, preferred_element_type=F32))

    def down_second(k, j):
        for which in range(NA):
            hidden = h_all[slot_of(k, j)]
            store_part(k, j, which, lax.dot_general(hidden, down_all[z, which], COL_COL, preferred_element_type=F32))

    def up_step(block, index, squares):
        block = block.reshape(NA * rows, slab).astype(F32)
        scaled = (block * gain_all[index]).astype(BF16)
        for which in range(NA):
            acc_h[...] += lax.dot_general(
                scaled[:, which * cols : (which + 1) * cols], up_all[index, which], ROW_ROW, preferred_element_type=F32
            )
        return squares + jnp.sum(block * block, axis=1, keepdims=True)

    def finish_hidden(squares):
        inverse_rms = lax.rsqrt(squares * (1.0 / (NT * slab)) + EPS)
        hidden = jax.nn.gelu(acc_h[...] * inverse_rms, approximate=True).astype(BF16)
        h_own[...] = hidden
        h_all[z] = hidden.T

    no_squares = jnp.zeros((NA * rows, 1), F32)

    def gain_wait():
        own_gain.wait()
        for o in range(1, NT):
            _, sy, sb = source(o)
            remote(gain, gain_all.at[sy * NB + sb], gain_send.at[o], gain_recv.at[o], **peer(o)).wait_recv()

    ahead = lax.rem(t - z + NZ, NZ)
    own_k = jnp.minimum(ahead, NZ - ahead)
    own_j = 1 - jnp.minimum(lax.rem(ahead + NZ - 1, NZ) // 3, 1)
    own_states = x1_all.at[own_k, pl.ds(pl.multiple_of(NT * a, NT), NT), own_j]
    back = remote(own_states, final, back_send, back_recv, section=1 - s)

    def final_copy(k, j):
        n = 2 * k + j
        return remote(
            sums.at[k, j], final.at[t], f_send.at[n], f_recv.at[t], z=slot_of(k, j), y=z // NB, b=lax.rem(z, NB)
        )

    final_local = pltpu.make_async_copy(sums.at[0, 0], final.at[t], f_recv.at[t])

    def gradient():
        acc_g[...] = jnp.zeros_like(acc_g)

        @pl.loop(0, NZ)
        def _(index):
            block = c_all[:, index // 4, lax.rem(index, 4)].reshape(NP * sub, slab)
            acc_g[...] += jnp.dot(h_all[index], block, preferred_element_type=F32)

        g_send[...] = acc_g[...].astype(BF16)

    swap = remote(g_send.at[:, their_cols], g_recv, g_ssem, g_rsem, a=other_a)

    @pl.when(first)
    def _():
        x_plane.start()
        for r in (0, 1):
            up_ring.start(r)
        for o in range(1, NT):
            gain_copy(o).start()
        from_up.wait_recv()
        for r in (2, 3):
            up_ring.start(r)
        ex_down.start()
        up_ring.arrive(0)
        up_ring.arrive(1)
        x_plane.relay()
        for r in range(2, up_ring.count):
            up_ring.arrive(r)
        own_down.wait()
        from_down.wait_recv()
        for r in range(4):
            down_ring.start(r)
        own_x[0].wait()
        own_x[1].wait()
        x_plane.wait()
        gain_wait()
        acc_h[...] = jnp.zeros_like(acc_h)
        finish_hidden(lax.fori_loop(0, NT, lambda i, squares: up_step(x_all[:, i], i, squares), no_squares))

        def residual(index):
            return x_all[a, index, t // 4, pl.ds(pl.multiple_of(lax.rem(t, 4) * sub, sub), sub), :].astype(F32)

        for k in range(STEPS):
            if k:
                down_ring.arrive_step(k)
            for j in range(width(k)):
                down_first(k, j)
            rs_start(k)
            if k == STEPS - 1:
                pl.semaphore_signal(gate, inc=1, device_id={"section": 1 - s}, device_id_type=MESH)
            if k >= 2:
                rs_sum(k - 2, residual)
                ag_start(k - 2)
        for k in (STEPS - 2, STEPS - 1):
            rs_sum(k, residual)
            ag_start(k)
        cz_start()
        h_ring.start(0)
        h_ring.start(1)
        cz_wait()
        own_c.start()
        c_plane.start()
        h_ring.arrive(0)
        h_ring.arrive(1)
        c_plane.relay()
        for r in range(2, h_ring.count):
            h_ring.arrive(r)
        own_c.wait()
        c_plane.wait()
        gradient()
        swap.start()
        back.wait_recv()
        states[...] = final[...].reshape(rows, slab)

    @pl.when(second)
    def _():
        cz_start()
        for o in range(1, NT):
            gain_copy(o).start()
        ex_down.start()
        cz_wait()
        own_c.start()
        c_plane.start()
        c_plane.relay()
        from_up.wait_recv()
        own_down.wait()
        from_down.wait_recv()
        gain_wait()
        pl.semaphore_wait(gate, 1)
        for r in range(4):
            up_ring.start(r)
        for r in range(up_ring.count):
            up_ring.arrive(r)
        acc_h[...] = jnp.zeros_like(acc_h)
        squares = no_squares
        for k in range(STEPS):
            ag_wait(k)
            for j in range(width(k)):
                squares = up_step(x1_all[k, :, j], slot_of(k, j), squares)
        finish_hidden(squares)
        back.start()
        h_ring.start(0)
        h_ring.start(1)
        for k in range(STEPS):
            if k:
                h_ring.arrive_step(k)
            for j in range(width(k)):
                down_second(k, j)
            rs_start(k)

        own_c.wait()
        c_plane.wait()
        gradient()
        swap.start()
        at_home = (z == t)
        for k in range(STEPS):
            rs_sum(k, None)
            for j in range(width(k)):
                if k:
                    final_copy(k, j).start()
                else:
                    @pl.when(at_home)
                    def _():
                        final_local.start()

                    @pl.when(jnp.logical_not(at_home))
                    def _():
                        final_copy(0, 0).start()
        for index in range(NT):
            pltpu.make_async_copy(final.at[index], final.at[index], f_recv.at[index]).wait()
        own_rows = x1_all[own_k, pl.ds(pl.multiple_of(NT * a, NT), NT), own_j].astype(F32)
        states[...] = (own_rows + final[...].astype(F32)).astype(BF16).reshape(rows, slab)

    grad[my_rows, :] = g_send[:, my_cols]
    swap.wait_recv()
    grad[their_rows, :] = g_recv[...]

    swap.wait_send()
    ex_up.wait_send()
    ex_down.wait_send()
    for o in range(1, NT):
        gain_copy(o).wait_send()
    for dz in range(1, NZ):
        cz_copy(dz).wait_send()
    for k in range(STEPS):
        for o in range(1, NP):
            rs_copy(k, o).wait_send()
    c_plane.drain()
    up_ring.drain()
    h_ring.drain()

    @pl.when(first)
    def _():
        x_plane.drain()
        down_ring.drain()
        for k in range(STEPS):
            for o in range(NP):
                ag_copy(k, o).wait_send()

    @pl.when(second)
    def _():
        back.wait_send()
        for k in range(STEPS):
            for j in range(width(k)):
                if k:
                    final_copy(k, j).wait_send()

        @pl.when(z != t)
        def _():
            final_copy(0, 0).wait_send()


def body(tokens, gain, w_up, w_down, cotangent):
    rows, slab = tokens.shape
    cols, hidden = w_up.shape[1:]
    half = hidden // 2
    sub = rows // NT
    dma = pltpu.SemaphoreType.DMA
    vmem = pl.BlockSpec(memory_space=pltpu.VMEM)
    states, grad = pl.pallas_call(
        kernel,
        out_shape=(
            jax.ShapeDtypeStruct((rows, slab), BF16),
            jax.ShapeDtypeStruct((hidden, cols), BF16),
        ),
        in_specs=[vmem] * 5,
        out_specs=(vmem, vmem),
        scratch_shapes=[
            pltpu.VMEM((NZ, NA, half, cols), BF16),
            pltpu.VMEM((NZ, NA, half, cols), BF16),
            pltpu.VMEM((NA, NT, 2, rows // 2, slab), BF16),
            pltpu.VMEM((STEPS, NP, 2, sub, slab), BF16),
            pltpu.VMEM((NZ, half, NA * rows), BF16),
            pltpu.VMEM((NA * rows, half), BF16),
            pltpu.VMEM((2, NZ // 2, sub, slab), BF16),
            pltpu.VMEM((NP, 2, NZ // 2, sub, slab), BF16),
            pltpu.VMEM((NT, 1, slab), F32),
            pltpu.VMEM((STEPS, NP, 2, sub, slab), BF16),
            pltpu.VMEM((STEPS, NP, 2, sub, slab), BF16),
            pltpu.VMEM((STEPS, 2, sub, slab), BF16),
            pltpu.VMEM((NT, sub, slab), BF16),
            pltpu.VMEM((NA * rows, half), F32),
            pltpu.VMEM((half, NA * cols), F32),
            pltpu.VMEM((half, NA * cols), BF16),
            pltpu.VMEM((half, cols), BF16),
            dma((2,)), dma((2,)), dma((7,)), dma((NT,)), dma((NT,)),
            dma((STEPS * NP,)), dma((STEPS * NP,)), dma((STEPS * NP,)), dma((STEPS * NP,)),
            dma((2 * STEPS,)), dma((NT,)), dma((NZ,)), dma((NZ,)), dma, dma, dma, dma,
        ]
        + [dma((14,))] * 8
        + [dma((7,))] * 4
        + [dma((6,)), dma((6,)), dma((24,)), dma((24,))] * 2
        + [pltpu.SemaphoreType.REGULAR],
        compiler_params=pltpu.CompilerParams(
            collective_id=0, has_side_effects=True, vmem_limit_bytes=48 * 1024 * 1024
        ),
    )(tokens, gain.astype(F32), w_up[0].T, w_down[0], cotangent[0])
    return states[None], grad[None]


def solution(mesh):
    torus = Mesh(
        mesh.devices.reshape(mesh.shape["section"], NZ, NA, NY, NB), ("section", "z", "a", "y", "b")
    )
    dp, tensor = ("z", "a"), ("y", "b")
    in_specs = (
        P(dp, tensor),
        P("section", tensor),
        P("section", dp, tensor),
        P("section", tensor, dp),
        P("section", dp, None),
    )
    out_specs = (P("section", dp, tensor), P("section", tensor, dp))
    return jax.shard_map(body, mesh=torus, in_specs=in_specs, out_specs=out_specs, check_vma=False)
```

```python
import jax
import jax.numpy as jnp
from jax import lax
from jax.experimental import pallas as pl
from jax.experimental.pallas import tpu as pltpu
from jax.sharding import Mesh
from jax.sharding import PartitionSpec as P

NZ, NA, NY, NB = 8, 2, 4, 2
NT = NY * NB
NP = NA * NT
STEPS = NZ // 2 + 1
GATE_STEP = 2
EPS = 1e-06
MESH = pl.DeviceIdType.MESH
F32 = jnp.float32
BF16 = jnp.bfloat16
OFFSETS = [(da, dy, db) for da in range(NA) for dy in range(NY) for db in range(NB)]
X_OFFSETS = [(1, 0, 0), (0, 0, 1), (1, 0, 1)]
Y_OFFSETS = [(0, dy, 0) for dy in range(1, NY)]
ROW_ROW = (((1,), (1,)), ((), ()))
COL_COL = (((0,), (0,)), ((), ()))


def remote(src, dst, send, recv, **where):
    return pltpu.make_async_remote_copy(
        src_ref=src, dst_ref=dst, send_sem=send, recv_sem=recv, device_id=where, device_id_type=MESH
    )


def wait_bytes(like, sem):
    pltpu.make_async_copy(like, like, sem).wait()


class Ring:
    COUNT = 14
    STEPS = ((0, 1, 2, 3), (4, 5, 6, 7), (8, 9, 10, 11), (12, 13))
    LEAD_STEPS = ((0, 1, 4, 5, 2, 3), (8, 9, 6, 7), (12, 10, 11), (13,))

    def __init__(self, z, piece, bulk, sems, steps=STEPS):
        self.z, self.piece, self.bulk, self.steps = z, piece, bulk, steps
        self.right_send, self.right_recv, self.left_send, self.left_recv = sems

    def _copy(self, origin, q, to_right, r):
        piece = self.piece(lax.rem(origin, NZ), q)
        if to_right:
            return remote(piece, piece, self.right_send, self.right_recv.at[r], z=lax.rem(self.z + 1, NZ))
        return remote(piece, piece, self.left_send, self.left_recv.at[r], z=lax.rem(self.z + NZ - 1, NZ))

    def _q(self, r, to_right):
        if r < 12:
            return r % 4
        return 2 * (r - 12) + (0 if to_right else 1)

    def right(self, r):
        return self._copy(self.z + NZ - r // 4, self._q(r, True), True, r)

    def left(self, r):
        return self._copy(self.z + r // 4, self._q(r, False), False, r)

    def start(self, r):
        self.right(r).start()
        self.left(r).start()

    def arrive(self, r):
        self._copy(self.z + 2 * NZ - 1 - r // 4, self._q(r, True), True, r).wait_recv()
        if r < 8:
            self.right(r + 4).start()
        elif r in (8, 10):
            self.right(12 + (r - 8) // 2).start()
        self._copy(self.z + 1 + r // 4, self._q(r, False), False, r).wait_recv()
        if r < 8:
            self.left(r + 4).start()
        elif r in (9, 11):
            self.left(12 + (r - 9) // 2).start()

    def arrive_step(self, k):
        for r in self.steps[k - 1]:
            self.arrive(r)

    def drain(self):
        wait_bytes(self.bulk, self.right_send)
        wait_bytes(self.bulk, self.left_send)


class Plane:
    def __init__(self, me, own, slot, bulk, sems):
        self.me, self.own, self.slot, self.bulk = me, own, slot, bulk
        self.send1, self.recv1, self.send2, self.recv2 = sems

    def _at(self, *offsets):
        a, y, b = self.me
        for da, dy, db in offsets:
            a, y, b = lax.rem(a + NA - da, NA), lax.rem(y + NY - dy, NY), lax.rem(b + NB - db, NB)
        return a, y, b

    def _peer(self, offset):
        a, y, b = self.me
        da, dy, db = offset
        return {"a": lax.rem(a + da, NA), "y": lax.rem(y + dy, NY), "b": lax.rem(b + db, NB)}

    def _first(self, half, i, origin):
        offset = (X_OFFSETS, Y_OFFSETS)[half][i]
        n = 3 * half + i
        return remote(self.own(half), self.slot(origin, half), self.send1, self.recv1.at[n], **self._peer(offset))

    def _second(self, half, i, piece, origin):
        offset = (Y_OFFSETS, X_OFFSETS)[half][i]
        return remote(piece, self.slot(origin, half), self.send2, self.recv2, **self._peer(offset))

    def start(self):
        for half in (0, 1):
            for i in range(3):
                self._first(half, i, self.me).start()
        for half in (0, 1):
            for i in range(3):
                self._second(half, i, self.own(half), self.me).start()

    def relay(self):
        for i in range(3):
            for half in (0, 1):
                origin = self._at((X_OFFSETS, Y_OFFSETS)[half][i])
                self._first(half, i, origin).wait_recv()
                piece = self.slot(origin, half)
                for n in range(3):
                    self._second(half, n, piece, origin).start()

    def wait(self):
        wait_bytes(self.bulk(24), self.recv2)

    def drain(self):
        wait_bytes(self.bulk(6), self.send1)
        wait_bytes(self.bulk(24), self.send2)


def kernel(
    tokens, gain, w_up, down, cot, states, grad,
    tok_v, gain_v, w_v, up_t, down_v, cot_v, squares,
    up_all, down_all, x_all, x1_all, h_all, h_own, c_z, c_all, gain_all, part_send, part_recv, sums, final,
    acc_h, acc_g, g_send, g_recv,
    ex_send, ex_recv, own_sem, gain_send, gain_recv, rs_send, rs_recv, ag_send, ag_recv, f_send, f_recv,
    cz_send, cz_recv, back_send, back_recv, g_ssem, g_rsem,
    u0, u1, u2, u3, d0, d1, d2, d3, h0, h1, h2, h3, x0, x1, x2, x3, c0, c1, c2, c3, gate,
):
    s = lax.axis_index("section")
    z = lax.axis_index("z")
    a = lax.axis_index("a")
    y = lax.axis_index("y")
    b = lax.axis_index("b")
    t = y * NB + b
    place = a * NT + t
    me = (a, y, b)
    first = s == 0
    second = s == 1
    half = w_up.shape[1] // 2
    cols = w_up.shape[0]
    rows, slab = tokens.shape
    sub = rows // NT
    other_a = 1 - a

    def peer(o):
        da, dy, db = OFFSETS[o]
        return {"a": lax.rem(a + da, NA), "y": lax.rem(y + dy, NY), "b": lax.rem(b + db, NB)}

    def source(o):
        da, dy, db = OFFSETS[o]
        return lax.rem(a + NA - da, NA), lax.rem(y + NY - dy, NY), lax.rem(b + NB - db, NB)

    my_rows = pl.ds(pl.multiple_of(half * a, half), half)
    their_rows = pl.ds(pl.multiple_of(half * other_a, half), half)
    my_cols = pl.ds(pl.multiple_of(cols * a, cols), cols)
    their_cols = pl.ds(pl.multiple_of(cols * other_a, cols), cols)
    cot_rows = pl.ds(pl.multiple_of(sub * t, sub), sub)

    def cot_cols(index):
        return pl.ds(pl.multiple_of(slab * index, slab), slab)

    def c_slot(index):
        return c_z.at[index // 4, lax.rem(index, 4)]

    load_w = pltpu.make_async_copy(w_up, w_v, own_sem.at[0])
    load_tok = pltpu.make_async_copy(tokens, tok_v, own_sem.at[1])
    own_x = [
        pltpu.make_async_copy(tokens.at[pl.ds(rows // 2 * i, rows // 2), :], x_all.at[a, t, i], own_sem.at[2 + i])
        for i in (0, 1)
    ]
    load_gain = pltpu.make_async_copy(gain, gain_v, own_sem.at[4])
    load_down = pltpu.make_async_copy(down.at[their_rows, :], down_v, own_sem.at[5])
    own_down = pltpu.make_async_copy(down.at[my_rows, :], down_all.at[z, a], own_sem.at[6])
    load_cot = pltpu.make_async_copy(cot.at[cot_rows, :], cot_v, own_sem.at[7])
    own_cot = pltpu.make_async_copy(cot.at[cot_rows, cot_cols(z)], c_slot(z), own_sem.at[8])
    own_c = pltpu.make_async_copy(c_z, c_all.at[place], own_sem.at[9])
    load_w.start()

    @pl.when(first)
    def _():
        load_tok.start()

    barrier = pltpu.get_barrier_semaphore()
    for dz in range(1, NZ):
        pl.semaphore_signal(barrier, inc=1, device_id={"z": lax.rem(z + dz, NZ)}, device_id_type=MESH)
    for offset in X_OFFSETS + Y_OFFSETS:
        pl.semaphore_signal(barrier, inc=1, device_id=peer(OFFSETS.index(offset)), device_id_type=MESH)
    pl.semaphore_signal(barrier, inc=1, device_id={"section": 1 - s}, device_id_type=MESH)

    @pl.when(first)
    def _():
        own_x[0].start()
        own_x[1].start()

    load_gain.start()
    load_down.start()
    own_down.start()
    load_cot.start()
    own_cot.start()
    load_w.wait()
    up_t[...] = w_v[...].T
    up_all[z, a] = up_t[my_rows, :]
    load_gain.wait()
    gain_all[t] = gain_v[...].astype(F32)

    @pl.when(first)
    def _():
        load_tok.wait()

    pl.semaphore_wait(barrier, NZ - 1 + len(X_OFFSETS) + len(Y_OFFSETS) + 1)

    quarter_rows = half // 2

    def ex_up(i):
        rows_there = pl.ds(pl.multiple_of(half * other_a + quarter_rows * i, quarter_rows), quarter_rows)
        landing = up_all.at[z, a, pl.ds(quarter_rows * i, quarter_rows), :]
        return remote(up_t.at[rows_there, :], landing, ex_send.at[i], ex_recv.at[i], a=other_a)

    def from_up(i):
        landing = up_all.at[z, other_a, pl.ds(quarter_rows * i, quarter_rows), :]
        return remote(landing, landing, ex_send.at[i], ex_recv.at[i], a=other_a)

    ex_down = remote(down_v, down_all.at[z, a], ex_send.at[2], ex_recv.at[2], a=other_a)
    from_down = remote(down_v, down_all.at[z, other_a], ex_send.at[2], ex_recv.at[2], a=other_a)


    def quarter(buffer):
        def piece(origin, q):
            which = a if q < 2 else other_a
            return buffer.at[origin, which, pl.ds(q % 2 * quarter_rows, quarter_rows), :]

        return piece

    up_ring = Ring(z, quarter(up_all), up_all.at[pl.ds(0, 7), 0], (u0, u1, u2, u3), Ring.LEAD_STEPS)
    down_ring = Ring(z, quarter(down_all), down_all.at[pl.ds(0, 7), 0], (d0, d1, d2, d3))
    h_rows = half // 4
    h_ring = Ring(
        z,
        lambda origin, q: h_all.at[origin, pl.ds(q * h_rows, h_rows), :],
        h_all.at[pl.ds(0, 7), pl.ds(0, 2 * h_rows), :],
        (h0, h1, h2, h3),
    )
    x_plane = Plane(
        me,
        lambda i: tok_v.at[pl.ds(rows // 2 * i, rows // 2), :],
        lambda at, i: x_all.at[at[0], at[1] * NB + at[2], i],
        lambda n: x_all.at[:, pl.ds(0, n // 4)] if n == 24 else x_all.at[0, pl.ds(0, n // 2)],
        (x0, x1, x2, x3),
    )
    c_plane = Plane(
        me,
        lambda i: c_z.at[i],
        lambda at, i: c_all.at[at[0] * NT + at[1] * NB + at[2], i],
        lambda n: c_all.at[pl.ds(0, n // 2)],
        (c0, c1, c2, c3),
    )

    gain_pair = gain_all.at[pl.ds(NB * y, NB)]

    def gain_copy(n):
        if n == 0:
            return remote(gain_all.at[t], gain_all.at[t], gain_send.at[0], gain_recv.at[0], b=1 - b)
        return remote(gain_pair, gain_pair, gain_send.at[n], gain_recv.at[n], y=lax.rem(y + n, NY))

    def gain_relay():
        other = gain_all.at[NB * y + 1 - b]
        remote(other, other, gain_send.at[0], gain_recv.at[0], b=1 - b).wait_recv()
        for n in range(1, NY):
            gain_copy(n).start()

    def gain_wait():
        for n in range(1, NY):
            pair = gain_all.at[pl.ds(NB * lax.rem(y + NY - n, NY), NB)]
            remote(pair, pair, gain_send.at[n], gain_recv.at[n], y=lax.rem(y + n, NY)).wait_recv()

    def cz_copy(dz):
        to = lax.rem(z + dz, NZ)
        return remote(cot_v.at[:, cot_cols(to)], c_slot(z), cz_send, cz_recv, z=to)

    def cz_start():
        load_cot.wait()
        for dz in range(1, NZ):
            cz_copy(dz).start()

    cz_bulk = cot_v.at[:, pl.ds(0, (NZ - 1) * slab)]

    def cz_wait():
        own_cot.wait()
        wait_bytes(cz_bulk, cz_recv)

    def width(k):
        return 2 if 0 < k < NZ // 2 else 1

    def slot_of(k, j):
        return lax.rem(z + (k if j else NZ - k), NZ)

    def view(buffer, k, *index):
        return buffer.at[(k, *index)] if width(k) == 2 else buffer.at[(k, *index, 0)]

    def rs_copy(k, o):
        to = peer(o)
        there = to["a"] * NT + to["y"] * NB + to["b"]
        return remote(view(part_send, k, there), view(part_recv, k, o), rs_send.at[k], rs_recv.at[k], **to)

    def rs_bulk(k):
        return view(part_recv, k, pl.ds(1, NP - 1))

    def rs_start(k):
        for o in range(1, NP):
            rs_copy(k, o).start()

    def rs_sum(k, extra):
        wait_bytes(rs_bulk(k), rs_recv.at[k])
        for j in range(width(k)):
            total = part_send[k, place, j].astype(F32)
            if extra is not None:
                total = total + extra(slot_of(k, j))
            for o in range(1, NP):
                total = total + part_recv[k, o, j].astype(F32)
            sums[k, j] = total.astype(BF16)

    def ag_copy(k, o):
        return remote(view(sums, k), view(x1_all, k, place), ag_send.at[k], ag_recv.at[k], section=1, **peer(o))

    def ag_bulk(k):
        return view(x1_all, k, slice(None))

    def ag_start(k):
        for o in range(NP):
            ag_copy(k, o).start()

    def ag_wait(k):
        wait_bytes(ag_bulk(k), ag_recv.at[k])

    def store_part(k, j, which, product):
        part_send[k, :, j, :, pl.ds(which * cols, cols)] = product.astype(BF16).reshape(NP, sub, cols)

    def down_first(k, j):
        for which in range(NA):
            weights = down_all[slot_of(k, j), which]
            store_part(k, j, which, jnp.dot(h_own[...], weights, preferred_element_type=F32))

    def down_second(k, j):
        for which in range(NA):
            hidden = h_all[slot_of(k, j)]
            store_part(k, j, which, lax.dot_general(hidden, down_all[z, which], COL_COL, preferred_element_type=F32))

    def up_start():
        acc_h[...] = jnp.zeros_like(acc_h)
        squares[...] = jnp.zeros_like(squares)

    def up_step(block, index):
        block = block.reshape(NA * rows, slab).astype(F32)
        scaled = (block * gain_all[index]).astype(BF16)
        for which in range(NA):
            acc_h[...] += lax.dot_general(
                scaled[:, which * cols : (which + 1) * cols], up_all[index, which], ROW_ROW, preferred_element_type=F32
            )
        squares[...] += jnp.sum(block * block, axis=1, keepdims=True)

    def finish_hidden():
        inverse_rms = lax.rsqrt(squares[...] * (1.0 / (NT * slab)) + EPS)
        hidden = jax.nn.gelu(acc_h[...] * inverse_rms, approximate=True).astype(BF16)
        h_own[...] = hidden
        h_all[z] = hidden.T

    ahead = lax.rem(t - z + NZ, NZ)
    own_k = jnp.minimum(ahead, NZ - ahead)
    own_j = 1 - jnp.minimum(lax.rem(ahead + NZ - 1, NZ) // 3, 1)
    own_states = x1_all.at[own_k, pl.ds(pl.multiple_of(NT * a, NT), NT), own_j]
    back = remote(own_states, final, back_send, back_recv, section=1 - s)

    def final_copy(k, j):
        return remote(
            sums.at[k, j], final.at[t], f_send.at[min(k, 1)], f_recv, z=slot_of(k, j), y=z // NB, b=lax.rem(z, NB)
        )

    final_local = pltpu.make_async_copy(sums.at[0, 0], final.at[t], f_recv)

    def gradient():
        acc_g[...] = jnp.zeros_like(acc_g)

        @pl.loop(0, NZ)
        def _(index):
            block = c_all[:, index // 4, lax.rem(index, 4)].reshape(NP * sub, slab)
            acc_g[...] += jnp.dot(h_all[index], block, preferred_element_type=F32)

        g_send[...] = acc_g[...].astype(BF16)

    swap = remote(g_send.at[:, their_cols], g_recv, g_ssem, g_rsem, a=other_a)

    @pl.when(first)
    def _():
        ex_up(0).start()
        ex_up(1).start()
        up_ring.start(0)
        up_ring.start(1)
        gain_copy(0).start()
        x_plane.start()
        cz_start()
        up_ring.arrive(0)
        up_ring.arrive(1)
        from_up(0).wait_recv()
        up_ring.start(2)
        from_up(1).wait_recv()
        up_ring.start(3)
        load_down.wait()
        ex_down.start()
        gain_relay()
        x_plane.relay()
        pl.semaphore_signal(gate.at[0], inc=1, device_id={"section": 1 - s}, device_id_type=MESH)
        up_ring.arrive(4)
        up_ring.arrive(5)
        cz_wait()
        own_c.start()
        c_plane.start()
        up_ring.arrive(2)
        up_ring.arrive(3)
        up_start()
        up_ring.arrive_step(2)
        own_x[0].wait()
        own_x[1].wait()
        gain_wait()
        up_ring.arrive_step(3)
        own_down.wait()
        from_down.wait_recv()
        for r in range(4):
            down_ring.start(r)
        x_plane.wait()

        def up_slots(k):
            for j in range(width(k)):
                up_step(x_all[:, slot_of(k, j)], slot_of(k, j))

        up_slots(0)
        up_slots(1)
        up_slots(2)
        up_slots(3)
        up_ring.arrive_step(4)
        up_slots(4)
        finish_hidden()

        def residual(index):
            return x_all[a, index, t // 4, pl.ds(pl.multiple_of(lax.rem(t, 4) * sub, sub), sub), :].astype(F32)

        for k in range(STEPS):
            if k:
                down_ring.arrive_step(k)
            if k == GATE_STEP:
                pl.semaphore_signal(gate.at[1], inc=1, device_id={"section": 1 - s}, device_id_type=MESH)
            for j in range(width(k)):
                down_first(k, j)
            rs_start(k)
            if k == 0:
                c_plane.relay()
            if k >= 2:
                rs_sum(k - 2, residual)
                ag_start(k - 2)
        for r in range(4):
            h_ring.start(r)
        rs_sum(STEPS - 2, residual)
        ag_start(STEPS - 2)
        h_ring.arrive_step(1)
        rs_sum(STEPS - 1, residual)
        ag_start(STEPS - 1)
        for k in range(2, STEPS):
            h_ring.arrive_step(k)
        own_c.wait()
        c_plane.wait()
        gradient()
        swap.start()
        back.wait_recv()
        states[...] = final[...].reshape(rows, slab)

    @pl.when(second)
    def _():
        gain_copy(0).start()
        load_down.wait()
        up_start()
        gain_relay()
        pl.semaphore_wait(gate.at[0], 1)
        ex_up(0).start()
        ex_up(1).start()
        ex_down.start()
        cz_start()
        cz_wait()
        own_c.start()
        c_plane.start()
        c_plane.relay()
        own_down.wait()
        from_up(0).wait_recv()
        from_up(1).wait_recv()
        from_down.wait_recv()
        gain_wait()
        pl.semaphore_wait(gate.at[1], 1)
        for r in range(4):
            up_ring.start(r)

        def up_slots(k):
            ag_wait(k)
            for j in range(width(k)):
                up_step(x1_all[k, :, j], slot_of(k, j))

        up_ring.arrive_step(1)
        up_ring.arrive_step(2)
        up_slots(0)
        up_ring.arrive_step(3)
        up_slots(1)
        up_ring.arrive_step(4)
        up_slots(2)
        up_slots(3)
        up_slots(4)
        finish_hidden()
        for r in range(4):
            h_ring.start(r)
        back.start()
        for k in range(STEPS):
            if k:
                h_ring.arrive_step(k)
            for j in range(width(k)):
                down_second(k, j)
            rs_start(k)

        own_c.wait()
        c_plane.wait()
        gradient()
        swap.start()
        at_home = (z == t)
        for k in range(STEPS):
            rs_sum(k, None)
            for j in range(width(k)):
                if k:
                    final_copy(k, j).start()
                else:
                    @pl.when(at_home)
                    def _():
                        final_local.start()

                    @pl.when(jnp.logical_not(at_home))
                    def _():
                        final_copy(0, 0).start()
        wait_bytes(final, f_recv)
        own_rows = x1_all[own_k, pl.ds(pl.multiple_of(NT * a, NT), NT), own_j].astype(F32)
        states[...] = (own_rows + final[...].astype(F32)).astype(BF16).reshape(rows, slab)

    grad[my_rows, :] = g_send[:, my_cols]
    swap.wait_recv()
    grad[their_rows, :] = g_recv[...]

    swap.wait_send()
    ex_up(0).wait_send()
    ex_up(1).wait_send()
    ex_down.wait_send()
    for n in range(NY):
        gain_copy(n).wait_send()
    wait_bytes(cz_bulk, cz_send)
    for k in range(STEPS):
        wait_bytes(rs_bulk(k), rs_send.at[k])
    c_plane.drain()
    up_ring.drain()
    h_ring.drain()

    @pl.when(first)
    def _():
        x_plane.drain()
        down_ring.drain()
        for k in range(STEPS):
            wait_bytes(ag_bulk(k), ag_send.at[k])

    @pl.when(second)
    def _():
        back.wait_send()
        wait_bytes(final.at[pl.ds(0, NZ - 1)], f_send.at[1])

        @pl.when(z != t)
        def _():
            final_copy(0, 0).wait_send()


def body(tokens, gain, w_up, w_down, cotangent):
    rows, slab = tokens.shape
    cols, hidden = w_up.shape[1:]
    half = hidden // 2
    sub = rows // NT
    dma = pltpu.SemaphoreType.DMA
    vmem = pl.BlockSpec(memory_space=pltpu.VMEM)
    states, grad = pl.pallas_call(
        kernel,
        out_shape=(
            jax.ShapeDtypeStruct((rows, slab), BF16),
            jax.ShapeDtypeStruct((hidden, cols), BF16),
        ),
        in_specs=[pl.BlockSpec(memory_space=pltpu.HBM)] * 5,
        out_specs=(vmem, vmem),
        scratch_shapes=[
            pltpu.VMEM((rows, slab), BF16),
            pltpu.VMEM((1, slab), BF16),
            pltpu.VMEM((cols, hidden), BF16),
            pltpu.VMEM((hidden, cols), BF16),
            pltpu.VMEM((half, cols), BF16),
            pltpu.VMEM((sub, NT * slab), BF16),
            pltpu.VMEM((NA * rows, 1), F32),
            pltpu.VMEM((NZ, NA, half, cols), BF16),
            pltpu.VMEM((NZ, NA, half, cols), BF16),
            pltpu.VMEM((NA, NT, 2, rows // 2, slab), BF16),
            pltpu.VMEM((STEPS, NP, 2, sub, slab), BF16),
            pltpu.VMEM((NZ, half, NA * rows), BF16),
            pltpu.VMEM((NA * rows, half), BF16),
            pltpu.VMEM((2, NZ // 2, sub, slab), BF16),
            pltpu.VMEM((NP, 2, NZ // 2, sub, slab), BF16),
            pltpu.VMEM((NT, 1, slab), F32),
            pltpu.VMEM((STEPS, NP, 2, sub, slab), BF16),
            pltpu.VMEM((STEPS, NP, 2, sub, slab), BF16),
            pltpu.VMEM((STEPS, 2, sub, slab), BF16),
            pltpu.VMEM((NT, sub, slab), BF16),
            pltpu.VMEM((NA * rows, half), F32),
            pltpu.VMEM((half, NA * cols), F32),
            pltpu.VMEM((half, NA * cols), BF16),
            pltpu.VMEM((half, cols), BF16),
            dma((3,)), dma((3,)), dma((10,)), dma((NY,)), dma((NY,)),
            dma((STEPS,)), dma((STEPS,)), dma((STEPS,)), dma((STEPS,)),
            dma((2,)), dma, dma, dma, dma, dma, dma, dma,
        ]
        + [dma, dma((Ring.COUNT,)), dma, dma((Ring.COUNT,))] * 3
        + [dma, dma((6,)), dma, dma] * 2
        + [pltpu.SemaphoreType.REGULAR((2,))],
        compiler_params=pltpu.CompilerParams(
            collective_id=0, has_side_effects=True, vmem_limit_bytes=66 * 1000 * 1000
        ),
    )(tokens, gain, w_up[0], w_down[0], cotangent[0])
    return states[None], grad[None]


def solution(mesh):
    torus = Mesh(
        mesh.devices.reshape(mesh.shape["section"], NZ, NA, NY, NB), ("section", "z", "a", "y", "b")
    )
    dp, tensor = ("z", "a"), ("y", "b")
    in_specs = (
        P(dp, tensor),
        P("section", tensor),
        P("section", dp, tensor),
        P("section", tensor, dp),
        P("section", dp, None),
    )
    out_specs = (P("section", dp, tensor), P("section", tensor, dp))
    return jax.shard_map(body, mesh=torus, in_specs=in_specs, out_specs=out_specs, check_vma=False)
```

```python
import jax
import jax.numpy as jnp
from jax import lax
from jax.experimental import pallas as pl
from jax.experimental.pallas import tpu as pltpu
from jax.sharding import Mesh
from jax.sharding import PartitionSpec as P

NZ, NA, NY, NB = 8, 2, 4, 2
NT = NY * NB
NP = NA * NT
STEPS = NZ // 2 + 1
GATE_STEP = 2
EPS = 1e-06
MESH = pl.DeviceIdType.MESH
F32 = jnp.float32
BF16 = jnp.bfloat16
OFFSETS = [(da, dy, db) for da in range(NA) for dy in range(NY) for db in range(NB)]
X_OFFSETS = [(1, 0, 0), (0, 0, 1), (1, 0, 1)]
Y_OFFSETS = [(0, dy, 0) for dy in range(1, NY)]
ROW_ROW = (((1,), (1,)), ((), ()))
COL_COL = (((0,), (0,)), ((), ()))


def remote(src, dst, send, recv, **where):
    return pltpu.make_async_remote_copy(
        src_ref=src, dst_ref=dst, send_sem=send, recv_sem=recv, device_id=where, device_id_type=MESH
    )


def wait_bytes(like, sem):
    pltpu.make_async_copy(like, like, sem).wait()


class Ring:
    COUNT = 14
    STEPS = ((0, 1, 2, 3), (4, 5, 6, 7), (8, 9, 10, 11), (12, 13))
    LEAD_STEPS = ((0, 1, 4, 5, 2, 3), (8, 9, 6, 7), (12, 10, 11), (13,))

    def __init__(self, z, piece, bulk, sems, steps=STEPS):
        self.z, self.piece, self.bulk, self.steps = z, piece, bulk, steps
        self.right_send, self.right_recv, self.left_send, self.left_recv = sems

    def _copy(self, origin, q, to_right, r):
        piece = self.piece(lax.rem(origin, NZ), q)
        if to_right:
            return remote(piece, piece, self.right_send, self.right_recv.at[r], z=lax.rem(self.z + 1, NZ))
        return remote(piece, piece, self.left_send, self.left_recv.at[r], z=lax.rem(self.z + NZ - 1, NZ))

    def _q(self, r, to_right):
        if r < 12:
            return r % 4
        return 2 * (r - 12) + (0 if to_right else 1)

    def right(self, r):
        return self._copy(self.z + NZ - r // 4, self._q(r, True), True, r)

    def left(self, r):
        return self._copy(self.z + r // 4, self._q(r, False), False, r)

    def start(self, r):
        self.right(r).start()
        self.left(r).start()

    def arrive(self, r):
        self._copy(self.z + 2 * NZ - 1 - r // 4, self._q(r, True), True, r).wait_recv()
        if r < 8:
            self.right(r + 4).start()
        elif r in (8, 10):
            self.right(12 + (r - 8) // 2).start()
        self._copy(self.z + 1 + r // 4, self._q(r, False), False, r).wait_recv()
        if r < 8:
            self.left(r + 4).start()
        elif r in (9, 11):
            self.left(12 + (r - 9) // 2).start()

    def arrive_step(self, k):
        for r in self.steps[k - 1]:
            self.arrive(r)

    def drain(self):
        wait_bytes(self.bulk, self.right_send)
        wait_bytes(self.bulk, self.left_send)


class Plane:
    def __init__(self, me, own, slot, bulk, sems):
        self.me, self.own, self.slot, self.bulk = me, own, slot, bulk
        self.send1, self.recv1, self.send2, self.recv2 = sems

    def _at(self, *offsets):
        a, y, b = self.me
        for da, dy, db in offsets:
            a, y, b = lax.rem(a + NA - da, NA), lax.rem(y + NY - dy, NY), lax.rem(b + NB - db, NB)
        return a, y, b

    def _peer(self, offset):
        a, y, b = self.me
        da, dy, db = offset
        return {"a": lax.rem(a + da, NA), "y": lax.rem(y + dy, NY), "b": lax.rem(b + db, NB)}

    def _first(self, half, i, origin):
        offset = (X_OFFSETS, Y_OFFSETS)[half][i]
        n = 3 * half + i
        return remote(self.own(half), self.slot(origin, half), self.send1, self.recv1.at[n], **self._peer(offset))

    def _second(self, half, i, piece, origin):
        offset = (Y_OFFSETS, X_OFFSETS)[half][i]
        return remote(piece, self.slot(origin, half), self.send2, self.recv2, **self._peer(offset))

    def start(self):
        for half in (0, 1):
            for i in range(3):
                self._first(half, i, self.me).start()
        for half in (0, 1):
            for i in range(3):
                self._second(half, i, self.own(half), self.me).start()

    def relay(self):
        for i in range(3):
            for half in (0, 1):
                origin = self._at((X_OFFSETS, Y_OFFSETS)[half][i])
                self._first(half, i, origin).wait_recv()
                piece = self.slot(origin, half)
                for n in range(3):
                    self._second(half, n, piece, origin).start()

    def wait(self):
        wait_bytes(self.bulk(24), self.recv2)

    def drain(self):
        wait_bytes(self.bulk(6), self.send1)
        wait_bytes(self.bulk(24), self.send2)


def kernel(
    tokens, gain, w_up, down, cot, states, grad,
    tok_v, gain_v, w_v, up_t, down_v, cot_v, squares,
    up_all, up_b, down_own, x_all, x1_all, h_all, c_z, c_all, gain_all, part_send, part_recv, sums, z_in, whole, final,
    acc_h, acc_g, g_send, g_recv,
    ex_send, ex_recv, bx_send, bx_recv, b_send, b_recv, z_send, z_recv, own_sem, gain_send, gain_recv, rs_send, rs_recv, ag_send, ag_recv, f_send, f_recv,
    cz_send, cz_recv, back_send, back_recv, g_ssem, g_rsem,
    u0, u1, u2, u3, a0, a1, a2, a3, h0, h1, h2, h3, x0, x1, x2, x3, c0, c1, c2, c3, gate,
):
    s = lax.axis_index("section")
    z = lax.axis_index("z")
    a = lax.axis_index("a")
    y = lax.axis_index("y")
    b = lax.axis_index("b")
    t = y * NB + b
    place = a * NT + t
    me = (a, y, b)
    first = s == 0
    second = s == 1
    half = w_up.shape[1] // 2
    cols = w_up.shape[0]
    rows, slab = tokens.shape
    sub = rows // NT
    other_a = 1 - a

    def peer(o):
        da, dy, db = OFFSETS[o]
        return {"a": lax.rem(a + da, NA), "y": lax.rem(y + dy, NY), "b": lax.rem(b + db, NB)}

    def source(o):
        da, dy, db = OFFSETS[o]
        return lax.rem(a + NA - da, NA), lax.rem(y + NY - dy, NY), lax.rem(b + NB - db, NB)

    my_rows = pl.ds(pl.multiple_of(half * a, half), half)
    their_rows = pl.ds(pl.multiple_of(half * other_a, half), half)
    my_cols = pl.ds(pl.multiple_of(cols * a, cols), cols)
    their_cols = pl.ds(pl.multiple_of(cols * other_a, cols), cols)
    cot_rows = pl.ds(pl.multiple_of(sub * t, sub), sub)

    def cot_cols(index):
        return pl.ds(pl.multiple_of(slab * index, slab), slab)

    def c_slot(index):
        return c_z.at[index // 4, lax.rem(index, 4)]

    load_w = pltpu.make_async_copy(w_up, w_v, own_sem.at[0])
    load_tok = pltpu.make_async_copy(tokens, tok_v, own_sem.at[1])
    own_x = [
        pltpu.make_async_copy(tokens.at[pl.ds(rows // 2 * i, rows // 2), :], x_all.at[a, t, i], own_sem.at[2 + i])
        for i in (0, 1)
    ]
    load_gain = pltpu.make_async_copy(gain, gain_v, own_sem.at[4])
    load_down = pltpu.make_async_copy(down.at[their_rows, :], down_v, own_sem.at[5])
    own_down = pltpu.make_async_copy(down.at[my_rows, :], down_own.at[a], own_sem.at[6])
    load_cot = pltpu.make_async_copy(cot.at[cot_rows, :], cot_v, own_sem.at[7])
    own_cot = pltpu.make_async_copy(cot.at[cot_rows, cot_cols(z)], c_slot(z), own_sem.at[8])
    own_c = pltpu.make_async_copy(c_z, c_all.at[place], own_sem.at[9])
    load_w.start()

    @pl.when(first)
    def _():
        load_tok.start()

    barrier = pltpu.get_barrier_semaphore()
    for dz in range(1, NZ):
        pl.semaphore_signal(barrier, inc=1, device_id={"z": lax.rem(z + dz, NZ)}, device_id_type=MESH)
    for offset in X_OFFSETS + Y_OFFSETS:
        pl.semaphore_signal(barrier, inc=1, device_id=peer(OFFSETS.index(offset)), device_id_type=MESH)
    pl.semaphore_signal(barrier, inc=1, device_id={"section": 1 - s}, device_id_type=MESH)

    @pl.when(second)
    def _():
        pl.semaphore_signal(barrier, inc=1, device_id={"section": 0, "a": other_a}, device_id_type=MESH)

    @pl.when(first)
    def _():
        own_x[0].start()
        own_x[1].start()

    load_gain.start()
    load_down.start()
    own_down.start()
    load_cot.start()
    own_cot.start()
    load_w.wait()
    up_t[...] = w_v[...].T
    up_all[z, a] = up_t[my_rows, :]
    load_gain.wait()
    gain_all[t] = gain_v[...].astype(F32)

    @pl.when(first)
    def _():
        load_tok.wait()

    greeted = NZ - 1 + len(X_OFFSETS) + len(Y_OFFSETS) + 1

    @pl.when(first)
    def _():
        pl.semaphore_wait(barrier, greeted + 1)

    @pl.when(second)
    def _():
        pl.semaphore_wait(barrier, greeted)

    quarter_rows = half // 2

    def ex_up(i):
        rows_there = pl.ds(pl.multiple_of(half * other_a + quarter_rows * i, quarter_rows), quarter_rows)
        landing = up_all.at[z, a, pl.ds(quarter_rows * i, quarter_rows), :]
        return remote(up_t.at[rows_there, :], landing, ex_send.at[i], ex_recv.at[i], a=other_a)

    def from_up(i):
        landing = up_all.at[z, other_a, pl.ds(quarter_rows * i, quarter_rows), :]
        return remote(landing, landing, ex_send.at[i], ex_recv.at[i], a=other_a)

    ex_down = remote(down_v, down_own.at[a], ex_send.at[2], ex_recv.at[2], a=other_a)
    from_down = remote(down_v, down_own.at[other_a], ex_send.at[2], ex_recv.at[2], a=other_a)

    b_rows = half // 4

    def bx_copy(q):
        rows_there = pl.ds(pl.multiple_of(half * other_a + b_rows * q, b_rows), b_rows)
        landing = up_b.at[z, pl.ds(b_rows * q, b_rows), :]
        return remote(up_t.at[rows_there, :], landing, bx_send, bx_recv.at[q], a=other_a, section=1)

    def bx_wait(q):
        landing = up_b.at[z, pl.ds(b_rows * q, b_rows), :]
        pltpu.make_async_copy(landing, landing, bx_recv.at[q]).wait()

    def b_copy(k, j):
        slot = lax.rem(z + (k if j else NZ - k), NZ)
        return remote(up_b.at[slot], up_all.at[slot, other_a], b_send, b_recv.at[k], section=0)

    def b_start(k):
        for j in range(2 if 0 < k < NZ // 2 else 1):
            b_copy(k, j).start()

    def b_wait(k):
        wait_bytes(up_b.at[pl.ds(0, 2 if 0 < k < NZ // 2 else 1)], b_recv.at[k])


    def quarter(buffer):
        def piece(origin, q):
            which = a if q < 2 else other_a
            return buffer.at[origin, which, pl.ds(q % 2 * quarter_rows, quarter_rows), :]

        return piece

    up_ring = Ring(z, quarter(up_all), up_all.at[pl.ds(0, 7), 0], (u0, u1, u2, u3), Ring.LEAD_STEPS)
    own_ring = Ring(
        z,
        lambda origin, q: up_all.at[origin, a, pl.ds(q * b_rows, b_rows), :],
        up_b.at[pl.ds(0, 7), pl.ds(0, 2 * b_rows), :],
        (a0, a1, a2, a3),
    )
    b_ring = Ring(
        z,
        lambda origin, q: up_b.at[origin, pl.ds(q * b_rows, b_rows), :],
        up_b.at[pl.ds(0, 7), pl.ds(0, 2 * b_rows), :],
        (a0, a1, a2, a3),
    )
    h_rows = half // 4
    h_ring = Ring(
        z,
        lambda origin, q: h_all.at[origin, pl.ds(q * h_rows, h_rows), :],
        h_all.at[pl.ds(0, 7), pl.ds(0, 2 * h_rows), :],
        (h0, h1, h2, h3),
    )
    x_plane = Plane(
        me,
        lambda i: tok_v.at[pl.ds(rows // 2 * i, rows // 2), :],
        lambda at, i: x_all.at[at[0], at[1] * NB + at[2], i],
        lambda n: x_all.at[:, pl.ds(0, n // 4)] if n == 24 else x_all.at[0, pl.ds(0, n // 2)],
        (x0, x1, x2, x3),
    )
    c_plane = Plane(
        me,
        lambda i: c_z.at[i],
        lambda at, i: c_all.at[at[0] * NT + at[1] * NB + at[2], i],
        lambda n: c_all.at[pl.ds(0, n // 2)],
        (c0, c1, c2, c3),
    )

    gain_pair = gain_all.at[pl.ds(NB * y, NB)]

    def gain_copy(n):
        if n == 0:
            return remote(gain_all.at[t], gain_all.at[t], gain_send.at[0], gain_recv.at[0], b=1 - b)
        return remote(gain_pair, gain_pair, gain_send.at[n], gain_recv.at[n], y=lax.rem(y + n, NY))

    def gain_relay():
        other = gain_all.at[NB * y + 1 - b]
        remote(other, other, gain_send.at[0], gain_recv.at[0], b=1 - b).wait_recv()
        for n in range(1, NY):
            gain_copy(n).start()

    def gain_wait():
        for n in range(1, NY):
            pair = gain_all.at[pl.ds(NB * lax.rem(y + NY - n, NY), NB)]
            remote(pair, pair, gain_send.at[n], gain_recv.at[n], y=lax.rem(y + n, NY)).wait_recv()

    def cz_copy(dz):
        to = lax.rem(z + dz, NZ)
        return remote(cot_v.at[:, cot_cols(to)], c_slot(z), cz_send, cz_recv, z=to)

    def cz_start():
        load_cot.wait()
        for dz in range(1, NZ):
            cz_copy(dz).start()

    cz_bulk = cot_v.at[:, pl.ds(0, (NZ - 1) * slab)]

    def cz_wait():
        own_cot.wait()
        wait_bytes(cz_bulk, cz_recv)

    def width(k):
        return 2 if 0 < k < NZ // 2 else 1

    def slot_of(k, j):
        return lax.rem(z + (k if j else NZ - k), NZ)

    def view(buffer, k, *index):
        return buffer.at[(k, *index)] if width(k) == 2 else buffer.at[(k, *index, 0)]

    def rs_copy(k, o):
        to = peer(o)
        there = to["a"] * NT + to["y"] * NB + to["b"]
        return remote(view(part_send, k, there), view(part_recv, k, o), rs_send.at[k], rs_recv.at[k], **to)

    def rs_bulk(k):
        return view(part_recv, k, pl.ds(1, NP - 1))

    def rs_start(k):
        for o in range(1, NP):
            rs_copy(k, o).start()

    def rs_sum(k):
        wait_bytes(rs_bulk(k), rs_recv.at[k])
        for j in range(width(k)):
            total = part_send[k, place, j].astype(F32)
            for o in range(1, NP):
                total = total + part_recv[k, o, j].astype(F32)
            sums[k, j] = total.astype(BF16)

    def z_copy(k, j):
        return remote(sums.at[k, j], z_in.at[k, width(k) - 1 - j], z_send, z_recv.at[k], z=slot_of(k, j))

    def z_start(k):
        for j in range(width(k)):
            if k:
                z_copy(k, j).start()

    def z_finish(k):
        if k:
            wait_bytes(view(z_in, k), z_recv.at[k])
        for j in range(width(k)):
            index = slot_of(k, j)
            before = x_all[a, index, t // 4, pl.ds(pl.multiple_of(lax.rem(t, 4) * sub, sub), sub), :]
            added = z_in[k, j] if k else sums[k, j]
            whole[k, j] = (before.astype(F32) + added.astype(F32)).astype(BF16)
        ag_start(k)

    def ag_copy(k, o):
        return remote(view(whole, k), view(x1_all, k, place), ag_send.at[k], ag_recv.at[k], section=1, **peer(o))

    def ag_bulk(k):
        return view(x1_all, k, slice(None))

    def ag_start(k):
        for o in range(NP):
            ag_copy(k, o).start()

    def ag_wait(k):
        wait_bytes(ag_bulk(k), ag_recv.at[k])

    def store_part(k, j, which, product):
        part_send[k, :, j, :, pl.ds(which * cols, cols)] = product.astype(BF16).reshape(NP, sub, cols)

    def down_product(k, j):
        for which in range(NA):
            hidden = h_all[slot_of(k, j)]
            store_part(k, j, which, lax.dot_general(hidden, down_own[which], COL_COL, preferred_element_type=F32))

    def up_start():
        acc_h[...] = jnp.zeros_like(acc_h)
        squares[...] = jnp.zeros_like(squares)

    def up_step(block, index):
        block = block.reshape(NA * rows, slab).astype(F32)
        scaled = (block * gain_all[index]).astype(BF16)
        for which in range(NA):
            acc_h[...] += lax.dot_general(
                scaled[:, which * cols : (which + 1) * cols], up_all[index, which], ROW_ROW, preferred_element_type=F32
            )
        squares[...] += jnp.sum(block * block, axis=1, keepdims=True)

    def finish_hidden():
        inverse_rms = lax.rsqrt(squares[...] * (1.0 / (NT * slab)) + EPS)
        hidden = jax.nn.gelu(acc_h[...] * inverse_rms, approximate=True).astype(BF16)
        h_all[z] = hidden.T

    ahead = lax.rem(t - z + NZ, NZ)
    own_k = jnp.minimum(ahead, NZ - ahead)
    own_j = 1 - jnp.minimum(lax.rem(ahead + NZ - 1, NZ) // 3, 1)
    own_states = x1_all.at[own_k, pl.ds(pl.multiple_of(NT * a, NT), NT), own_j]
    back = remote(own_states, final, back_send, back_recv, section=1 - s)

    def final_copy(k, j):
        return remote(
            sums.at[k, j], final.at[t], f_send.at[min(k, 1)], f_recv, z=slot_of(k, j), y=z // NB, b=lax.rem(z, NB)
        )

    final_local = pltpu.make_async_copy(sums.at[0, 0], final.at[t], f_recv)

    def gradient():
        acc_g[...] = jnp.zeros_like(acc_g)

        @pl.loop(0, NZ)
        def _(index):
            block = c_all[:, index // 4, lax.rem(index, 4)].reshape(NP * sub, slab)
            acc_g[...] += jnp.dot(h_all[index], block, preferred_element_type=F32)

        g_send[...] = acc_g[...].astype(BF16)

    swap = remote(g_send.at[:, their_cols], g_recv, g_ssem, g_rsem, a=other_a)

    @pl.when(first)
    def _():
        for q in range(4):
            bx_copy(q).start()
        for r in range(4):
            own_ring.start(r)
        gain_copy(0).start()
        x_plane.start()
        cz_start()
        own_ring.arrive_step(1)
        gain_relay()
        x_plane.relay()
        pl.semaphore_signal(gate.at[0], inc=1, device_id={"section": 1 - s}, device_id_type=MESH)
        load_down.wait()
        ex_down.start()
        cz_wait()
        own_c.start()
        c_plane.start()
        up_start()
        own_ring.arrive_step(2)
        own_x[0].wait()
        own_x[1].wait()
        gain_wait()
        own_ring.arrive_step(3)
        c_plane.relay()
        x_plane.wait()

        def up_slots(k):
            b_wait(k)
            for j in range(width(k)):
                up_step(x_all[:, slot_of(k, j)], slot_of(k, j))

        for k in range(STEPS - 1):
            up_slots(k)
        own_ring.arrive_step(4)
        up_slots(STEPS - 1)
        finish_hidden()
        own_down.wait()
        from_down.wait_recv()
        for r in range(4):
            h_ring.start(r)
        for k in range(STEPS):
            if k:
                h_ring.arrive_step(k)
            if k == GATE_STEP:
                pl.semaphore_signal(gate.at[1], inc=1, device_id={"section": 1 - s}, device_id_type=MESH)
            for j in range(width(k)):
                down_product(k, j)
            rs_start(k)
            if k >= 2:
                rs_sum(k - 2)
                z_start(k - 2)
            if k >= 3:
                z_finish(k - 3)
        rs_sum(STEPS - 2)
        z_start(STEPS - 2)
        z_finish(STEPS - 3)
        rs_sum(STEPS - 1)
        z_start(STEPS - 1)
        z_finish(STEPS - 2)
        z_finish(STEPS - 1)
        own_c.wait()
        c_plane.wait()
        gradient()
        swap.start()
        back.wait_recv()
        states[...] = final[...].reshape(rows, slab)

    @pl.when(second)
    def _():
        gain_copy(0).start()
        for q in range(4):
            bx_wait(q)
            b_ring.start(q)
        b_start(0)
        for k in range(1, STEPS):
            b_ring.arrive_step(k)
            b_start(k)
            if k == 1:
                cz_start()
                up_start()
            if k == 2:
                gain_relay()
                pl.semaphore_wait(gate.at[0], 1)
                cz_wait()
                own_c.start()
                c_plane.start()
                load_down.wait()
                ex_up(0).start()
                ex_up(1).start()
                ex_down.start()
            if k == 4:
                c_plane.relay()
        own_down.wait()
        from_up(0).wait_recv()
        from_up(1).wait_recv()
        from_down.wait_recv()
        gain_wait()
        pl.semaphore_wait(gate.at[1], 1)
        for r in range(4):
            up_ring.start(r)

        def up_slots(k):
            ag_wait(k)
            for j in range(width(k)):
                up_step(x1_all[k, :, j], slot_of(k, j))

        up_ring.arrive_step(1)
        up_ring.arrive_step(2)
        up_slots(0)
        up_ring.arrive_step(3)
        up_slots(1)
        up_ring.arrive_step(4)
        up_slots(2)
        up_slots(3)
        up_slots(4)
        finish_hidden()
        for r in range(4):
            h_ring.start(r)
        back.start()
        for k in range(STEPS):
            if k:
                h_ring.arrive_step(k)
            for j in range(width(k)):
                down_product(k, j)
            rs_start(k)

        own_c.wait()
        c_plane.wait()
        gradient()
        swap.start()
        at_home = (z == t)
        for k in range(STEPS):
            rs_sum(k)
            for j in range(width(k)):
                if k:
                    final_copy(k, j).start()
                else:
                    @pl.when(at_home)
                    def _():
                        final_local.start()

                    @pl.when(jnp.logical_not(at_home))
                    def _():
                        final_copy(0, 0).start()
        wait_bytes(final, f_recv)
        own_rows = x1_all[own_k, pl.ds(pl.multiple_of(NT * a, NT), NT), own_j].astype(F32)
        states[...] = (own_rows + final[...].astype(F32)).astype(BF16).reshape(rows, slab)

    grad[my_rows, :] = g_send[:, my_cols]
    swap.wait_recv()
    grad[their_rows, :] = g_recv[...]

    swap.wait_send()
    ex_down.wait_send()
    for n in range(NY):
        gain_copy(n).wait_send()
    wait_bytes(cz_bulk, cz_send)
    for k in range(STEPS):
        wait_bytes(rs_bulk(k), rs_send.at[k])
    c_plane.drain()
    own_ring.drain()
    h_ring.drain()

    @pl.when(first)
    def _():
        x_plane.drain()
        wait_bytes(up_b.at[0], bx_send)
        wait_bytes(final.at[pl.ds(0, NZ - 1)], z_send)
        for k in range(STEPS):
            wait_bytes(ag_bulk(k), ag_send.at[k])

    @pl.when(second)
    def _():
        back.wait_send()
        up_ring.drain()
        ex_up(0).wait_send()
        ex_up(1).wait_send()
        wait_bytes(up_b, b_send)
        wait_bytes(final.at[pl.ds(0, NZ - 1)], f_send.at[1])

        @pl.when(z != t)
        def _():
            final_copy(0, 0).wait_send()


def body(tokens, gain, w_up, w_down, cotangent):
    rows, slab = tokens.shape
    cols, hidden = w_up.shape[1:]
    half = hidden // 2
    sub = rows // NT
    dma = pltpu.SemaphoreType.DMA
    vmem = pl.BlockSpec(memory_space=pltpu.VMEM)
    states, grad = pl.pallas_call(
        kernel,
        out_shape=(
            jax.ShapeDtypeStruct((rows, slab), BF16),
            jax.ShapeDtypeStruct((hidden, cols), BF16),
        ),
        in_specs=[pl.BlockSpec(memory_space=pltpu.HBM)] * 5,
        out_specs=(vmem, vmem),
        scratch_shapes=[
            pltpu.VMEM((rows, slab), BF16),
            pltpu.VMEM((1, slab), BF16),
            pltpu.VMEM((cols, hidden), BF16),
            pltpu.VMEM((hidden, cols), BF16),
            pltpu.VMEM((half, cols), BF16),
            pltpu.VMEM((sub, NT * slab), BF16),
            pltpu.VMEM((NA * rows, 1), F32),
            pltpu.VMEM((NZ, NA, half, cols), BF16),
            pltpu.VMEM((NZ, half, cols), BF16),
            pltpu.VMEM((NA, half, cols), BF16),
            pltpu.VMEM((NA, NT, 2, rows // 2, slab), BF16),
            pltpu.VMEM((STEPS, NP, 2, sub, slab), BF16),
            pltpu.VMEM((NZ, half, NA * rows), BF16),
            pltpu.VMEM((2, NZ // 2, sub, slab), BF16),
            pltpu.VMEM((NP, 2, NZ // 2, sub, slab), BF16),
            pltpu.VMEM((NT, 1, slab), F32),
            pltpu.VMEM((STEPS, NP, 2, sub, slab), BF16),
            pltpu.VMEM((STEPS, NP, 2, sub, slab), BF16),
            pltpu.VMEM((STEPS, 2, sub, slab), BF16),
            pltpu.VMEM((STEPS, 2, sub, slab), BF16),
            pltpu.VMEM((STEPS, 2, sub, slab), BF16),
            pltpu.VMEM((NT, sub, slab), BF16),
            pltpu.VMEM((NA * rows, half), F32),
            pltpu.VMEM((half, NA * cols), F32),
            pltpu.VMEM((half, NA * cols), BF16),
            pltpu.VMEM((half, cols), BF16),
            dma((3,)), dma((3,)), dma, dma((4,)), dma, dma((STEPS,)), dma, dma((STEPS,)), dma((10,)), dma((NY,)), dma((NY,)),
            dma((STEPS,)), dma((STEPS,)), dma((STEPS,)), dma((STEPS,)),
            dma((2,)), dma, dma, dma, dma, dma, dma, dma,
        ]
        + [dma, dma((Ring.COUNT,)), dma, dma((Ring.COUNT,))] * 3
        + [dma, dma((6,)), dma, dma] * 2
        + [pltpu.SemaphoreType.REGULAR((2,))],
        compiler_params=pltpu.CompilerParams(
            collective_id=0, has_side_effects=True, vmem_limit_bytes=48 * 1024 * 1024
        ),
    )(*[pltpu.with_memory_space_constraint(x, pltpu.HBM) for x in (tokens, gain, w_up[0], w_down[0], cotangent[0])])
    return states[None], grad[None]


def solution(mesh):
    torus = Mesh(
        mesh.devices.reshape(mesh.shape["section"], NZ, NA, NY, NB), ("section", "z", "a", "y", "b")
    )
    dp, tensor = ("z", "a"), ("y", "b")
    in_specs = (
        P(dp, tensor),
        P("section", tensor),
        P("section", dp, tensor),
        P("section", tensor, dp),
        P("section", dp, None),
    )
    out_specs = (P("section", dp, tensor), P("section", tensor, dp))
    return jax.shard_map(body, mesh=torus, in_specs=in_specs, out_specs=out_specs, check_vma=False)
```

```python
import jax
import jax.numpy as jnp
from jax import lax
from jax.experimental import pallas as pl
from jax.experimental.pallas import tpu as pltpu
from jax.sharding import Mesh
from jax.sharding import PartitionSpec as P

NZ, NA, NY, NB = 8, 2, 4, 2
NT = NY * NB
NP = NA * NT
STEPS = NZ // 2 + 1
GATE_STEP = 2
EPS = 1e-06
MESH = pl.DeviceIdType.MESH
F32 = jnp.float32
BF16 = jnp.bfloat16
OFFSETS = [(da, dy, db) for da in range(NA) for dy in range(NY) for db in range(NB)]
X_OFFSETS = [(1, 0, 0), (0, 0, 1), (1, 0, 1)]
Y_OFFSETS = [(0, dy, 0) for dy in range(1, NY)]
ROW_ROW = (((1,), (1,)), ((), ()))
COL_COL = (((0,), (0,)), ((), ()))


def remote(src, dst, send, recv, **where):
    return pltpu.make_async_remote_copy(
        src_ref=src, dst_ref=dst, send_sem=send, recv_sem=recv, device_id=where, device_id_type=MESH
    )


def wait_bytes(like, sem):
    pltpu.make_async_copy(like, like, sem).wait()


class Ring:
    COUNT = 14
    STEPS = ((0, 1, 2, 3), (4, 5, 6, 7), (8, 9, 10, 11), (12, 13))
    LEAD_STEPS = ((0, 1, 4, 5, 2, 3), (8, 9, 6, 7), (12, 10, 11), (13,))

    def __init__(self, z, piece, bulk, sems, steps=STEPS):
        self.z, self.piece, self.bulk, self.steps = z, piece, bulk, steps
        self.right_send, self.right_recv, self.left_send, self.left_recv = sems

    def _copy(self, origin, q, to_right, r):
        piece = self.piece(lax.rem(origin, NZ), q)
        if to_right:
            return remote(piece, piece, self.right_send, self.right_recv.at[r], z=lax.rem(self.z + 1, NZ))
        return remote(piece, piece, self.left_send, self.left_recv.at[r], z=lax.rem(self.z + NZ - 1, NZ))

    def _q(self, r, to_right):
        if r < 12:
            return r % 4
        return 2 * (r - 12) + (0 if to_right else 1)

    def right(self, r):
        return self._copy(self.z + NZ - r // 4, self._q(r, True), True, r)

    def left(self, r):
        return self._copy(self.z + r // 4, self._q(r, False), False, r)

    def start(self, r):
        self.right(r).start()
        self.left(r).start()

    def arrive(self, r):
        self._copy(self.z + 2 * NZ - 1 - r // 4, self._q(r, True), True, r).wait_recv()
        if r < 8:
            self.right(r + 4).start()
        elif r in (8, 10):
            self.right(12 + (r - 8) // 2).start()
        self._copy(self.z + 1 + r // 4, self._q(r, False), False, r).wait_recv()
        if r < 8:
            self.left(r + 4).start()
        elif r in (9, 11):
            self.left(12 + (r - 9) // 2).start()

    def arrive_step(self, k):
        for r in self.steps[k - 1]:
            self.arrive(r)

    def drain(self):
        wait_bytes(self.bulk, self.right_send)
        wait_bytes(self.bulk, self.left_send)


class Plane:
    def __init__(self, me, own, slot, bulk, sems):
        self.me, self.own, self.slot, self.bulk = me, own, slot, bulk
        self.send1, self.recv1, self.send2, self.recv2 = sems

    def _at(self, *offsets):
        a, y, b = self.me
        for da, dy, db in offsets:
            a, y, b = lax.rem(a + NA - da, NA), lax.rem(y + NY - dy, NY), lax.rem(b + NB - db, NB)
        return a, y, b

    def _peer(self, offset):
        a, y, b = self.me
        da, dy, db = offset
        return {"a": lax.rem(a + da, NA), "y": lax.rem(y + dy, NY), "b": lax.rem(b + db, NB)}

    def _first(self, half, i, origin):
        offset = (X_OFFSETS, Y_OFFSETS)[half][i]
        n = 3 * half + i
        return remote(self.own(half), self.slot(origin, half), self.send1, self.recv1.at[n], **self._peer(offset))

    def _second(self, half, i, piece, origin):
        offset = (Y_OFFSETS, X_OFFSETS)[half][i]
        return remote(piece, self.slot(origin, half), self.send2, self.recv2, **self._peer(offset))

    def start(self):
        for half in (0, 1):
            for i in range(3):
                self._first(half, i, self.me).start()
        for half in (0, 1):
            for i in range(3):
                self._second(half, i, self.own(half), self.me).start()

    def relay(self):
        for i in range(3):
            for half in (0, 1):
                origin = self._at((X_OFFSETS, Y_OFFSETS)[half][i])
                self._first(half, i, origin).wait_recv()
                piece = self.slot(origin, half)
                for n in range(3):
                    self._second(half, n, piece, origin).start()

    def wait(self):
        wait_bytes(self.bulk(24), self.recv2)

    def drain(self):
        wait_bytes(self.bulk(6), self.send1)
        wait_bytes(self.bulk(24), self.send2)


def kernel(
    tokens, gain, w_up, down, cot, states, grad,
    tok_v, gain_v, w_v, up_t, down_v, cot_v, squares,
    up_all, up_b, down_own, x_all, x1_all, h_all, c_z, c_all, gain_all, part_send, part_recv, sums, z_in, whole, final,
    acc_h, acc_g, g_send, g_recv,
    ex_send, ex_recv, bx_send, bx_recv, b_send, b_recv, z_send, z_recv, own_sem, gain_send, gain_recv, rs_send, rs_recv, ag_send, ag_recv, f_send, f_recv,
    cz_send, cz_recv, back_send, back_recv, g_ssem, g_rsem,
    u0, u1, u2, u3, a0, a1, a2, a3, h0, h1, h2, h3, x0, x1, x2, x3, c0, c1, c2, c3, gate,
):
    s = lax.axis_index("section")
    z = lax.axis_index("z")
    a = lax.axis_index("a")
    y = lax.axis_index("y")
    b = lax.axis_index("b")
    t = y * NB + b
    place = a * NT + t
    me = (a, y, b)
    first = s == 0
    second = s == 1
    half = w_up.shape[1] // 2
    cols = w_up.shape[0]
    rows, slab = tokens.shape
    sub = rows // NT
    other_a = 1 - a

    def peer(o):
        da, dy, db = OFFSETS[o]
        return {"a": lax.rem(a + da, NA), "y": lax.rem(y + dy, NY), "b": lax.rem(b + db, NB)}

    def source(o):
        da, dy, db = OFFSETS[o]
        return lax.rem(a + NA - da, NA), lax.rem(y + NY - dy, NY), lax.rem(b + NB - db, NB)

    my_rows = pl.ds(pl.multiple_of(half * a, half), half)
    their_rows = pl.ds(pl.multiple_of(half * other_a, half), half)
    my_cols = pl.ds(pl.multiple_of(cols * a, cols), cols)
    their_cols = pl.ds(pl.multiple_of(cols * other_a, cols), cols)
    cot_rows = pl.ds(pl.multiple_of(sub * t, sub), sub)

    def cot_cols(index):
        return pl.ds(pl.multiple_of(slab * index, slab), slab)

    def c_slot(index):
        return c_z.at[index // 4, lax.rem(index, 4)]

    load_w = pltpu.make_async_copy(w_up, w_v, own_sem.at[0])
    load_tok = pltpu.make_async_copy(tokens, tok_v, own_sem.at[1])
    own_x = [
        pltpu.make_async_copy(tokens.at[pl.ds(rows // 2 * i, rows // 2), :], x_all.at[a, t, i], own_sem.at[2 + i])
        for i in (0, 1)
    ]
    load_gain = pltpu.make_async_copy(gain, gain_v, own_sem.at[4])
    load_down = pltpu.make_async_copy(down.at[their_rows, :], down_v, own_sem.at[5])
    own_down = pltpu.make_async_copy(down.at[my_rows, :], down_own.at[a], own_sem.at[6])
    load_cot = pltpu.make_async_copy(cot.at[cot_rows, :], cot_v, own_sem.at[7])
    own_cot = pltpu.make_async_copy(cot.at[cot_rows, cot_cols(z)], c_slot(z), own_sem.at[8])
    own_c = pltpu.make_async_copy(c_z, c_all.at[place], own_sem.at[9])
    load_w.start()

    @pl.when(first)
    def _():
        load_tok.start()

    barrier = pltpu.get_barrier_semaphore()
    for dz in range(1, NZ):
        pl.semaphore_signal(barrier, inc=1, device_id={"z": lax.rem(z + dz, NZ)}, device_id_type=MESH)
    for offset in X_OFFSETS + Y_OFFSETS:
        pl.semaphore_signal(barrier, inc=1, device_id=peer(OFFSETS.index(offset)), device_id_type=MESH)
    pl.semaphore_signal(barrier, inc=1, device_id={"section": 1 - s}, device_id_type=MESH)

    @pl.when(second)
    def _():
        pl.semaphore_signal(barrier, inc=1, device_id={"section": 0, "a": other_a}, device_id_type=MESH)

    @pl.when(first)
    def _():
        own_x[0].start()
        own_x[1].start()

    load_gain.start()
    load_down.start()
    own_down.start()
    load_cot.start()
    own_cot.start()
    load_w.wait()
    up_t[...] = w_v[...].T
    up_all[z, a] = up_t[my_rows, :]
    load_gain.wait()
    gain_all[t] = gain_v[...].astype(F32)

    @pl.when(first)
    def _():
        load_tok.wait()

    greeted = NZ - 1 + len(X_OFFSETS) + len(Y_OFFSETS) + 1

    @pl.when(first)
    def _():
        pl.semaphore_wait(barrier, greeted + 1)

    @pl.when(second)
    def _():
        pl.semaphore_wait(barrier, greeted)

    quarter_rows = half // 2

    def ex_up(i):
        rows_there = pl.ds(pl.multiple_of(half * other_a + quarter_rows * i, quarter_rows), quarter_rows)
        landing = up_all.at[z, a, pl.ds(quarter_rows * i, quarter_rows), :]
        return remote(up_t.at[rows_there, :], landing, ex_send.at[i], ex_recv.at[i], a=other_a)

    def from_up(i):
        landing = up_all.at[z, other_a, pl.ds(quarter_rows * i, quarter_rows), :]
        return remote(landing, landing, ex_send.at[i], ex_recv.at[i], a=other_a)

    ex_down = remote(down_v, down_own.at[a], ex_send.at[2], ex_recv.at[2], a=other_a)
    from_down = remote(down_v, down_own.at[other_a], ex_send.at[2], ex_recv.at[2], a=other_a)

    b_rows = half // 4

    def bx_copy(q):
        rows_there = pl.ds(pl.multiple_of(half * other_a + b_rows * q, b_rows), b_rows)
        landing = up_b.at[z, pl.ds(b_rows * q, b_rows), :]
        return remote(up_t.at[rows_there, :], landing, bx_send, bx_recv.at[q], a=other_a, section=1)

    def bx_wait(q):
        landing = up_b.at[z, pl.ds(b_rows * q, b_rows), :]
        pltpu.make_async_copy(landing, landing, bx_recv.at[q]).wait()

    def b_copy(k, j):
        slot = lax.rem(z + (k if j else NZ - k), NZ)
        return remote(up_b.at[slot], up_all.at[slot, other_a], b_send, b_recv.at[k], section=0)

    def b_start(k):
        for j in range(2 if 0 < k < NZ // 2 else 1):
            b_copy(k, j).start()

    def b_wait(k):
        wait_bytes(up_b.at[pl.ds(0, 2 if 0 < k < NZ // 2 else 1)], b_recv.at[k])


    def quarter(buffer):
        def piece(origin, q):
            which = a if q < 2 else other_a
            return buffer.at[origin, which, pl.ds(q % 2 * quarter_rows, quarter_rows), :]

        return piece

    up_ring = Ring(z, quarter(up_all), up_all.at[pl.ds(0, 7), 0], (u0, u1, u2, u3), Ring.LEAD_STEPS)
    own_ring = Ring(
        z,
        lambda origin, q: up_all.at[origin, a, pl.ds(q * b_rows, b_rows), :],
        up_b.at[pl.ds(0, 7), pl.ds(0, 2 * b_rows), :],
        (a0, a1, a2, a3),
    )
    b_ring = Ring(
        z,
        lambda origin, q: up_b.at[origin, pl.ds(q * b_rows, b_rows), :],
        up_b.at[pl.ds(0, 7), pl.ds(0, 2 * b_rows), :],
        (a0, a1, a2, a3),
    )
    h_rows = half // 4
    h_ring = Ring(
        z,
        lambda origin, q: h_all.at[origin, pl.ds(q * h_rows, h_rows), :],
        h_all.at[pl.ds(0, 7), pl.ds(0, 2 * h_rows), :],
        (h0, h1, h2, h3),
    )
    x_plane = Plane(
        me,
        lambda i: tok_v.at[pl.ds(rows // 2 * i, rows // 2), :],
        lambda at, i: x_all.at[at[0], at[1] * NB + at[2], i],
        lambda n: x_all.at[:, pl.ds(0, n // 4)] if n == 24 else x_all.at[0, pl.ds(0, n // 2)],
        (x0, x1, x2, x3),
    )
    c_plane = Plane(
        me,
        lambda i: c_z.at[i],
        lambda at, i: c_all.at[at[0] * NT + at[1] * NB + at[2], i],
        lambda n: c_all.at[pl.ds(0, n // 2)],
        (c0, c1, c2, c3),
    )

    gain_pair = gain_all.at[pl.ds(NB * y, NB)]

    def gain_copy(n):
        if n == 0:
            return remote(gain_all.at[t], gain_all.at[t], gain_send.at[0], gain_recv.at[0], b=1 - b)
        return remote(gain_pair, gain_pair, gain_send.at[n], gain_recv.at[n], y=lax.rem(y + n, NY))

    def gain_relay():
        other = gain_all.at[NB * y + 1 - b]
        remote(other, other, gain_send.at[0], gain_recv.at[0], b=1 - b).wait_recv()
        for n in range(1, NY):
            gain_copy(n).start()

    def gain_wait():
        for n in range(1, NY):
            pair = gain_all.at[pl.ds(NB * lax.rem(y + NY - n, NY), NB)]
            remote(pair, pair, gain_send.at[n], gain_recv.at[n], y=lax.rem(y + n, NY)).wait_recv()

    def cz_copy(dz):
        to = lax.rem(z + dz, NZ)
        return remote(cot_v.at[:, cot_cols(to)], c_slot(z), cz_send, cz_recv, z=to)

    def cz_start():
        load_cot.wait()
        for dz in range(1, NZ):
            cz_copy(dz).start()

    cz_bulk = cot_v.at[:, pl.ds(0, (NZ - 1) * slab)]

    def cz_wait():
        own_cot.wait()
        wait_bytes(cz_bulk, cz_recv)

    def width(k):
        return 2 if 0 < k < NZ // 2 else 1

    def slot_of(k, j):
        return lax.rem(z + (k if j else NZ - k), NZ)

    def view(buffer, k, *index):
        return buffer.at[(k, *index)] if width(k) == 2 else buffer.at[(k, *index, 0)]

    def rs_copy(k, o):
        to = peer(o)
        there = to["a"] * NT + to["y"] * NB + to["b"]
        return remote(view(part_send, k, there), view(part_recv, k, o), rs_send.at[k], rs_recv.at[k], **to)

    def rs_bulk(k):
        return view(part_recv, k, pl.ds(1, NP - 1))

    def rs_start(k):
        for o in range(1, NP):
            rs_copy(k, o).start()

    def rs_sum(k):
        wait_bytes(rs_bulk(k), rs_recv.at[k])
        for j in range(width(k)):
            total = part_send[k, place, j].astype(F32)
            for o in range(1, NP):
                total = total + part_recv[k, o, j].astype(F32)
            sums[k, j] = total.astype(BF16)

    def z_copy(k, j):
        return remote(sums.at[k, j], z_in.at[k, width(k) - 1 - j], z_send, z_recv.at[k], z=slot_of(k, j))

    def z_start(k):
        for j in range(width(k)):
            if k:
                z_copy(k, j).start()

    def z_finish(k):
        if k:
            wait_bytes(view(z_in, k), z_recv.at[k])
        for j in range(width(k)):
            index = slot_of(k, j)
            before = x_all[a, index, t // 4, pl.ds(pl.multiple_of(lax.rem(t, 4) * sub, sub), sub), :]
            added = z_in[k, j] if k else sums[k, j]
            whole[k, j] = (before.astype(F32) + added.astype(F32)).astype(BF16)
        ag_start(k)

    def ag_copy(k, o):
        return remote(view(whole, k), view(x1_all, k, place), ag_send.at[k], ag_recv.at[k], section=1, **peer(o))

    def ag_bulk(k):
        return view(x1_all, k, slice(None))

    def ag_start(k):
        for o in range(NP):
            ag_copy(k, o).start()

    def ag_wait(k):
        wait_bytes(ag_bulk(k), ag_recv.at[k])

    def store_part(k, j, which, product):
        part_send[k, :, j, :, pl.ds(which * cols, cols)] = product.astype(BF16).reshape(NP, sub, cols)

    def down_product(k, j):
        for which in range(NA):
            hidden = h_all[slot_of(k, j)]
            store_part(k, j, which, lax.dot_general(hidden, down_own[which], COL_COL, preferred_element_type=F32))

    def up_start():
        acc_h[...] = jnp.zeros_like(acc_h)
        squares[...] = jnp.zeros_like(squares)

    def up_step(block, index):
        block = block.reshape(NA * rows, slab).astype(F32)
        scaled = (block * gain_all[index]).astype(BF16)
        for which in range(NA):
            acc_h[...] += lax.dot_general(
                scaled[:, which * cols : (which + 1) * cols], up_all[index, which], ROW_ROW, preferred_element_type=F32
            )
        squares[...] += jnp.sum(block * block, axis=1, keepdims=True)

    def finish_hidden():
        inverse_rms = lax.rsqrt(squares[...] * (1.0 / (NT * slab)) + EPS)
        hidden = jax.nn.gelu(acc_h[...] * inverse_rms, approximate=True).astype(BF16)
        h_all[z] = hidden.T

    ahead = lax.rem(t - z + NZ, NZ)
    own_k = jnp.minimum(ahead, NZ - ahead)
    own_j = 1 - jnp.minimum(lax.rem(ahead + NZ - 1, NZ) // 3, 1)
    own_states = x1_all.at[own_k, pl.ds(pl.multiple_of(NT * a, NT), NT), own_j]
    back = remote(own_states, final, back_send, back_recv, section=1 - s)

    def final_copy(k, j):
        return remote(
            sums.at[k, j], final.at[t], f_send.at[min(k, 1)], f_recv, z=slot_of(k, j), y=z // NB, b=lax.rem(z, NB)
        )

    final_local = pltpu.make_async_copy(sums.at[0, 0], final.at[t], f_recv)

    def gradient():
        acc_g[...] = jnp.zeros_like(acc_g)

        @pl.loop(0, NZ)
        def _(index):
            block = c_all[:, index // 4, lax.rem(index, 4)].reshape(NP * sub, slab)
            acc_g[...] += jnp.dot(h_all[index], block, preferred_element_type=F32)

        g_send[...] = acc_g[...].astype(BF16)

    swap = remote(g_send.at[:, their_cols], g_recv, g_ssem, g_rsem, a=other_a)

    @pl.when(first)
    def _():
        for q in range(4):
            bx_copy(q).start()
        for r in range(4):
            own_ring.start(r)
        gain_copy(0).start()
        x_plane.start()
        own_ring.arrive_step(1)
        gain_relay()
        x_plane.relay()
        load_down.wait()
        ex_down.start()
        up_start()
        own_ring.arrive_step(2)
        own_x[0].wait()
        own_x[1].wait()
        gain_wait()
        own_ring.arrive_step(3)
        x_plane.wait()

        def up_slots(k):
            b_wait(k)
            for j in range(width(k)):
                up_step(x_all[:, slot_of(k, j)], slot_of(k, j))

        for k in range(STEPS - 1):
            up_slots(k)
        own_ring.arrive_step(4)
        up_slots(STEPS - 1)
        finish_hidden()
        own_down.wait()
        from_down.wait_recv()
        for r in range(4):
            h_ring.start(r)
        for k in range(STEPS):
            if k:
                h_ring.arrive_step(k)
            if k == GATE_STEP:
                pl.semaphore_signal(gate.at[1], inc=1, device_id={"section": 1 - s}, device_id_type=MESH)
            for j in range(width(k)):
                down_product(k, j)
            rs_start(k)
            if k >= 2:
                rs_sum(k - 2)
                z_start(k - 2)
            if k >= 3:
                z_finish(k - 3)
        cz_start()
        rs_sum(STEPS - 2)
        z_start(STEPS - 2)
        z_finish(STEPS - 3)
        rs_sum(STEPS - 1)
        z_start(STEPS - 1)
        z_finish(STEPS - 2)
        z_finish(STEPS - 1)
        cz_wait()
        own_c.start()
        c_plane.start()
        c_plane.relay()
        own_c.wait()
        c_plane.wait()
        gradient()
        swap.start()
        back.wait_recv()
        states[...] = final[...].reshape(rows, slab)

    @pl.when(second)
    def _():
        gain_copy(0).start()
        cz_start()
        for q in range(4):
            bx_wait(q)
            b_ring.start(q)
        b_start(0)
        for k in range(1, STEPS):
            b_ring.arrive_step(k)
            b_start(k)
            if k == 1:
                up_start()
                cz_wait()
                own_c.start()
                c_plane.start()
            if k == 2:
                gain_relay()
                load_down.wait()
                ex_up(0).start()
                ex_up(1).start()
                ex_down.start()
            if k == 3:
                c_plane.relay()
        own_down.wait()
        from_up(0).wait_recv()
        from_up(1).wait_recv()
        from_down.wait_recv()
        gain_wait()
        pl.semaphore_wait(gate.at[1], 1)
        for r in range(4):
            up_ring.start(r)

        def up_slots(k):
            ag_wait(k)
            for j in range(width(k)):
                up_step(x1_all[k, :, j], slot_of(k, j))

        up_ring.arrive_step(1)
        up_ring.arrive_step(2)
        up_slots(0)
        up_ring.arrive_step(3)
        up_slots(1)
        up_ring.arrive_step(4)
        up_slots(2)
        up_slots(3)
        up_slots(4)
        finish_hidden()
        for r in range(4):
            h_ring.start(r)
        back.start()
        for k in range(STEPS):
            if k:
                h_ring.arrive_step(k)
            for j in range(width(k)):
                down_product(k, j)
            rs_start(k)

        own_c.wait()
        c_plane.wait()
        gradient()
        swap.start()
        at_home = (z == t)
        for k in range(STEPS):
            rs_sum(k)
            for j in range(width(k)):
                if k:
                    final_copy(k, j).start()
                else:
                    @pl.when(at_home)
                    def _():
                        final_local.start()

                    @pl.when(jnp.logical_not(at_home))
                    def _():
                        final_copy(0, 0).start()
        wait_bytes(final, f_recv)
        own_rows = x1_all[own_k, pl.ds(pl.multiple_of(NT * a, NT), NT), own_j].astype(F32)
        states[...] = (own_rows + final[...].astype(F32)).astype(BF16).reshape(rows, slab)

    grad[my_rows, :] = g_send[:, my_cols]
    swap.wait_recv()
    grad[their_rows, :] = g_recv[...]

    swap.wait_send()
    ex_down.wait_send()
    for n in range(NY):
        gain_copy(n).wait_send()
    wait_bytes(cz_bulk, cz_send)
    for k in range(STEPS):
        wait_bytes(rs_bulk(k), rs_send.at[k])
    c_plane.drain()
    own_ring.drain()
    h_ring.drain()

    @pl.when(first)
    def _():
        x_plane.drain()
        wait_bytes(up_b.at[0], bx_send)
        wait_bytes(final.at[pl.ds(0, NZ - 1)], z_send)
        for k in range(STEPS):
            wait_bytes(ag_bulk(k), ag_send.at[k])

    @pl.when(second)
    def _():
        back.wait_send()
        up_ring.drain()
        ex_up(0).wait_send()
        ex_up(1).wait_send()
        wait_bytes(up_b, b_send)
        wait_bytes(final.at[pl.ds(0, NZ - 1)], f_send.at[1])

        @pl.when(z != t)
        def _():
            final_copy(0, 0).wait_send()


def body(tokens, gain, w_up, w_down, cotangent):
    rows, slab = tokens.shape
    cols, hidden = w_up.shape[1:]
    half = hidden // 2
    sub = rows // NT
    dma = pltpu.SemaphoreType.DMA
    vmem = pl.BlockSpec(memory_space=pltpu.VMEM)
    states, grad = pl.pallas_call(
        kernel,
        out_shape=(
            jax.ShapeDtypeStruct((rows, slab), BF16),
            jax.ShapeDtypeStruct((hidden, cols), BF16),
        ),
        in_specs=[pl.BlockSpec(memory_space=pltpu.HBM)] * 5,
        out_specs=(vmem, vmem),
        scratch_shapes=[
            pltpu.VMEM((rows, slab), BF16),
            pltpu.VMEM((1, slab), BF16),
            pltpu.VMEM((cols, hidden), BF16),
            pltpu.VMEM((hidden, cols), BF16),
            pltpu.VMEM((half, cols), BF16),
            pltpu.VMEM((sub, NT * slab), BF16),
            pltpu.VMEM((NA * rows, 1), F32),
            pltpu.VMEM((NZ, NA, half, cols), BF16),
            pltpu.VMEM((NZ, half, cols), BF16),
            pltpu.VMEM((NA, half, cols), BF16),
            pltpu.VMEM((NA, NT, 2, rows // 2, slab), BF16),
            pltpu.VMEM((STEPS, NP, 2, sub, slab), BF16),
            pltpu.VMEM((NZ, half, NA * rows), BF16),
            pltpu.VMEM((2, NZ // 2, sub, slab), BF16),
            pltpu.VMEM((NP, 2, NZ // 2, sub, slab), BF16),
            pltpu.VMEM((NT, 1, slab), F32),
            pltpu.VMEM((STEPS, NP, 2, sub, slab), BF16),
            pltpu.VMEM((STEPS, NP, 2, sub, slab), BF16),
            pltpu.VMEM((STEPS, 2, sub, slab), BF16),
            pltpu.VMEM((STEPS, 2, sub, slab), BF16),
            pltpu.VMEM((STEPS, 2, sub, slab), BF16),
            pltpu.VMEM((NT, sub, slab), BF16),
            pltpu.VMEM((NA * rows, half), F32),
            pltpu.VMEM((half, NA * cols), F32),
            pltpu.VMEM((half, NA * cols), BF16),
            pltpu.VMEM((half, cols), BF16),
            dma((3,)), dma((3,)), dma, dma((4,)), dma, dma((STEPS,)), dma, dma((STEPS,)), dma((10,)), dma((NY,)), dma((NY,)),
            dma((STEPS,)), dma((STEPS,)), dma((STEPS,)), dma((STEPS,)),
            dma((2,)), dma, dma, dma, dma, dma, dma, dma,
        ]
        + [dma, dma((Ring.COUNT,)), dma, dma((Ring.COUNT,))] * 3
        + [dma, dma((6,)), dma, dma] * 2
        + [pltpu.SemaphoreType.REGULAR((2,))],
        compiler_params=pltpu.CompilerParams(
            collective_id=0, has_side_effects=True, vmem_limit_bytes=48 * 1024 * 1024
        ),
    )(*[pltpu.with_memory_space_constraint(x, pltpu.HBM) for x in (tokens, gain, w_up[0], w_down[0], cotangent[0])])
    return states[None], grad[None]


def solution(mesh):
    torus = Mesh(
        mesh.devices.reshape(mesh.shape["section"], NZ, NA, NY, NB), ("section", "z", "a", "y", "b")
    )
    dp, tensor = ("z", "a"), ("y", "b")
    in_specs = (
        P(dp, tensor),
        P("section", tensor),
        P("section", dp, tensor),
        P("section", tensor, dp),
        P("section", dp, None),
    )
    out_specs = (P("section", dp, tensor), P("section", tensor, dp))
    return jax.shard_map(body, mesh=torus, in_specs=in_specs, out_specs=out_specs, check_vma=False)
```

```python
import jax
import jax.numpy as jnp
from jax import lax
from jax.experimental import pallas as pl
from jax.experimental.pallas import tpu as pltpu
from jax.sharding import Mesh
from jax.sharding import PartitionSpec as P

NZ, NA, NY, NB = 8, 2, 4, 2
NT = NY * NB
NP = NA * NT
STEPS = NZ // 2 + 1
GATE_STEP = 2
PAIRED = ((), (2, 3))
EPS = 1e-06
MESH = pl.DeviceIdType.MESH
F32 = jnp.float32
BF16 = jnp.bfloat16
OFFSETS = [(da, dy, db) for da in range(NA) for dy in range(NY) for db in range(NB)]
X_OFFSETS = [(1, 0, 0), (0, 0, 1), (1, 0, 1)]
Y_OFFSETS = [(0, dy, 0) for dy in range(1, NY)]
ROW_ROW = (((1,), (1,)), ((), ()))
COL_COL = (((0,), (0,)), ((), ()))


def remote(src, dst, send, recv, **where):
    return pltpu.make_async_remote_copy(
        src_ref=src, dst_ref=dst, send_sem=send, recv_sem=recv, device_id=where, device_id_type=MESH
    )


def wait_bytes(like, sem):
    pltpu.make_async_copy(like, like, sem).wait()


class Ring:
    COUNT = 14
    STEPS = ((0, 1, 2, 3), (4, 5, 6, 7), (8, 9, 10, 11), (12, 13))
    LEAD_STEPS = ((0, 1, 4, 5, 2, 3), (8, 9, 6, 7), (12, 10, 11), (13,))

    def __init__(self, z, piece, bulk, sems, steps=STEPS):
        self.z, self.piece, self.bulk, self.steps = z, piece, bulk, steps
        self.right_send, self.right_recv, self.left_send, self.left_recv = sems

    def _copy(self, origin, q, to_right, r):
        piece = self.piece(lax.rem(origin, NZ), q)
        if to_right:
            return remote(piece, piece, self.right_send, self.right_recv.at[r], z=lax.rem(self.z + 1, NZ))
        return remote(piece, piece, self.left_send, self.left_recv.at[r], z=lax.rem(self.z + NZ - 1, NZ))

    def _q(self, r, to_right):
        if r < 12:
            return r % 4
        return 2 * (r - 12) + (0 if to_right else 1)

    def right(self, r):
        return self._copy(self.z + NZ - r // 4, self._q(r, True), True, r)

    def left(self, r):
        return self._copy(self.z + r // 4, self._q(r, False), False, r)

    def start(self, r):
        self.right(r).start()
        self.left(r).start()

    def arrive(self, r):
        self._copy(self.z + 2 * NZ - 1 - r // 4, self._q(r, True), True, r).wait_recv()
        if r < 8:
            self.right(r + 4).start()
        elif r in (8, 10):
            self.right(12 + (r - 8) // 2).start()
        self._copy(self.z + 1 + r // 4, self._q(r, False), False, r).wait_recv()
        if r < 8:
            self.left(r + 4).start()
        elif r in (9, 11):
            self.left(12 + (r - 9) // 2).start()

    def arrive_step(self, k):
        for r in self.steps[k - 1]:
            self.arrive(r)

    def drain(self):
        wait_bytes(self.bulk, self.right_send)
        wait_bytes(self.bulk, self.left_send)


class Plane:
    def __init__(self, me, own, slot, bulk, sems):
        self.me, self.own, self.slot, self.bulk = me, own, slot, bulk
        self.send1, self.recv1, self.send2, self.recv2 = sems

    def _at(self, *offsets):
        a, y, b = self.me
        for da, dy, db in offsets:
            a, y, b = lax.rem(a + NA - da, NA), lax.rem(y + NY - dy, NY), lax.rem(b + NB - db, NB)
        return a, y, b

    def _peer(self, offset):
        a, y, b = self.me
        da, dy, db = offset
        return {"a": lax.rem(a + da, NA), "y": lax.rem(y + dy, NY), "b": lax.rem(b + db, NB)}

    def _first(self, half, i, origin):
        offset = (X_OFFSETS, Y_OFFSETS)[half][i]
        n = 3 * half + i
        return remote(self.own(half), self.slot(origin, half), self.send1, self.recv1.at[n], **self._peer(offset))

    def _second(self, half, i, piece, origin):
        offset = (Y_OFFSETS, X_OFFSETS)[half][i]
        return remote(piece, self.slot(origin, half), self.send2, self.recv2, **self._peer(offset))

    def start(self):
        for half in (0, 1):
            for i in range(3):
                self._first(half, i, self.me).start()
        for half in (0, 1):
            for i in range(3):
                self._second(half, i, self.own(half), self.me).start()

    def relay(self):
        for i in range(3):
            for half in (0, 1):
                origin = self._at((X_OFFSETS, Y_OFFSETS)[half][i])
                self._first(half, i, origin).wait_recv()
                piece = self.slot(origin, half)
                for n in range(3):
                    self._second(half, n, piece, origin).start()

    def wait(self):
        wait_bytes(self.bulk(24), self.recv2)

    def drain(self):
        wait_bytes(self.bulk(6), self.send1)
        wait_bytes(self.bulk(24), self.send2)


def kernel(
    tokens, gain, w_up, down, cot, states, grad,
    tok_v, gain_v, w_v, up_t, down_v, cot_v, squares,
    up_all, up_b, down_own, x_all, x1_all, h_all, c_z, c_all, gain_all, part_send, part_recv, row_in, col_in, row_out, col_out, row_last, col_last, sums, z_in, whole, final,
    acc_h, acc_g, g_send, g_recv,
    ex_send, ex_recv, bx_send, bx_recv, b_send, b_recv, z_send, z_recv, own_sem, gain_send, gain_recv, rs_send, rs_recv, mid_send, mid_recv, last_send, last_recv, ag_send, ag_recv, f_send, f_recv,
    cz_send, cz_recv, back_send, back_recv, g_ssem, g_rsem,
    u0, u1, u2, u3, a0, a1, a2, a3, h0, h1, h2, h3, x0, x1, x2, x3, c0, c1, c2, c3, gate,
):
    s = lax.axis_index("section")
    z = lax.axis_index("z")
    a = lax.axis_index("a")
    y = lax.axis_index("y")
    b = lax.axis_index("b")
    t = y * NB + b
    place = a * NT + t
    me = (a, y, b)
    first = s == 0
    second = s == 1
    half = w_up.shape[1] // 2
    cols = w_up.shape[0]
    rows, slab = tokens.shape
    sub = rows // NT
    other_a = 1 - a

    def peer(o):
        da, dy, db = OFFSETS[o]
        return {"a": lax.rem(a + da, NA), "y": lax.rem(y + dy, NY), "b": lax.rem(b + db, NB)}

    def source(o):
        da, dy, db = OFFSETS[o]
        return lax.rem(a + NA - da, NA), lax.rem(y + NY - dy, NY), lax.rem(b + NB - db, NB)

    my_rows = pl.ds(pl.multiple_of(half * a, half), half)
    their_rows = pl.ds(pl.multiple_of(half * other_a, half), half)
    my_cols = pl.ds(pl.multiple_of(cols * a, cols), cols)
    their_cols = pl.ds(pl.multiple_of(cols * other_a, cols), cols)
    cot_rows = pl.ds(pl.multiple_of(sub * t, sub), sub)

    def cot_cols(index):
        return pl.ds(pl.multiple_of(slab * index, slab), slab)

    def c_slot(index):
        return c_z.at[index // 4, lax.rem(index, 4)]

    load_w = pltpu.make_async_copy(w_up, w_v, own_sem.at[0])
    load_tok = pltpu.make_async_copy(tokens, tok_v, own_sem.at[1])
    own_x = [
        pltpu.make_async_copy(tokens.at[pl.ds(rows // 2 * i, rows // 2), :], x_all.at[a, t, i], own_sem.at[2 + i])
        for i in (0, 1)
    ]
    load_gain = pltpu.make_async_copy(gain, gain_v, own_sem.at[4])
    load_down = pltpu.make_async_copy(down.at[their_rows, :], down_v, own_sem.at[5])
    own_down = pltpu.make_async_copy(down.at[my_rows, :], down_own.at[a], own_sem.at[6])
    load_cot = pltpu.make_async_copy(cot.at[cot_rows, :], cot_v, own_sem.at[7])
    own_cot = pltpu.make_async_copy(cot.at[cot_rows, cot_cols(z)], c_slot(z), own_sem.at[8])
    own_c = pltpu.make_async_copy(c_z, c_all.at[place], own_sem.at[9])
    load_w.start()

    @pl.when(first)
    def _():
        load_tok.start()

    barrier = pltpu.get_barrier_semaphore()
    for dz in range(1, NZ):
        pl.semaphore_signal(barrier, inc=1, device_id={"z": lax.rem(z + dz, NZ)}, device_id_type=MESH)
    for offset in X_OFFSETS + Y_OFFSETS:
        pl.semaphore_signal(barrier, inc=1, device_id=peer(OFFSETS.index(offset)), device_id_type=MESH)
    pl.semaphore_signal(barrier, inc=1, device_id={"section": 1 - s}, device_id_type=MESH)

    @pl.when(second)
    def _():
        pl.semaphore_signal(barrier, inc=1, device_id={"section": 0, "a": other_a}, device_id_type=MESH)

    @pl.when(first)
    def _():
        own_x[0].start()
        own_x[1].start()

    load_gain.start()
    load_down.start()
    own_down.start()
    load_cot.start()
    own_cot.start()
    load_w.wait()
    up_t[...] = w_v[...].T
    up_all[z, a] = up_t[my_rows, :]
    load_gain.wait()
    gain_all[t] = gain_v[...].astype(F32)

    @pl.when(first)
    def _():
        load_tok.wait()

    greeted = NZ - 1 + len(X_OFFSETS) + len(Y_OFFSETS) + 1

    @pl.when(first)
    def _():
        pl.semaphore_wait(barrier, greeted + 1)

    @pl.when(second)
    def _():
        pl.semaphore_wait(barrier, greeted)

    quarter_rows = half // 2

    def ex_up(i):
        rows_there = pl.ds(pl.multiple_of(half * other_a + quarter_rows * i, quarter_rows), quarter_rows)
        landing = up_all.at[z, a, pl.ds(quarter_rows * i, quarter_rows), :]
        return remote(up_t.at[rows_there, :], landing, ex_send.at[i], ex_recv.at[i], a=other_a)

    def from_up(i):
        landing = up_all.at[z, other_a, pl.ds(quarter_rows * i, quarter_rows), :]
        return remote(landing, landing, ex_send.at[i], ex_recv.at[i], a=other_a)

    ex_down = remote(down_v, down_own.at[a], ex_send.at[2], ex_recv.at[2], a=other_a)
    from_down = remote(down_v, down_own.at[other_a], ex_send.at[2], ex_recv.at[2], a=other_a)

    b_rows = half // 4

    def bx_copy(q):
        rows_there = pl.ds(pl.multiple_of(half * other_a + b_rows * q, b_rows), b_rows)
        landing = up_b.at[z, pl.ds(b_rows * q, b_rows), :]
        return remote(up_t.at[rows_there, :], landing, bx_send, bx_recv.at[q], a=other_a, section=1)

    def bx_wait(q):
        landing = up_b.at[z, pl.ds(b_rows * q, b_rows), :]
        pltpu.make_async_copy(landing, landing, bx_recv.at[q]).wait()

    def b_copy(k, j):
        slot = lax.rem(z + (k if j else NZ - k), NZ)
        return remote(up_b.at[slot], up_all.at[slot, other_a], b_send, b_recv.at[k], section=0)

    def b_start(k):
        for j in range(2 if 0 < k < NZ // 2 else 1):
            b_copy(k, j).start()

    def b_wait(k):
        wait_bytes(up_b.at[pl.ds(0, 2 if 0 < k < NZ // 2 else 1)], b_recv.at[k])


    def quarter(buffer):
        def piece(origin, q):
            which = a if q < 2 else other_a
            return buffer.at[origin, which, pl.ds(q % 2 * quarter_rows, quarter_rows), :]

        return piece

    up_ring = Ring(z, quarter(up_all), up_all.at[pl.ds(0, 7), 0], (u0, u1, u2, u3), Ring.LEAD_STEPS)
    own_ring = Ring(
        z,
        lambda origin, q: up_all.at[origin, a, pl.ds(q * b_rows, b_rows), :],
        up_b.at[pl.ds(0, 7), pl.ds(0, 2 * b_rows), :],
        (a0, a1, a2, a3),
    )
    b_ring = Ring(
        z,
        lambda origin, q: up_b.at[origin, pl.ds(q * b_rows, b_rows), :],
        up_b.at[pl.ds(0, 7), pl.ds(0, 2 * b_rows), :],
        (a0, a1, a2, a3),
    )
    h_rows = half // 4
    h_ring = Ring(
        z,
        lambda origin, q: h_all.at[origin, pl.ds(q * h_rows, h_rows), :],
        h_all.at[pl.ds(0, 7), pl.ds(0, 2 * h_rows), :],
        (h0, h1, h2, h3),
    )
    x_plane = Plane(
        me,
        lambda i: tok_v.at[pl.ds(rows // 2 * i, rows // 2), :],
        lambda at, i: x_all.at[at[0], at[1] * NB + at[2], i],
        lambda n: x_all.at[:, pl.ds(0, n // 4)] if n == 24 else x_all.at[0, pl.ds(0, n // 2)],
        (x0, x1, x2, x3),
    )
    c_plane = Plane(
        me,
        lambda i: c_z.at[i],
        lambda at, i: c_all.at[at[0] * NT + at[1] * NB + at[2], i],
        lambda n: c_all.at[pl.ds(0, n // 2)],
        (c0, c1, c2, c3),
    )

    gain_pair = gain_all.at[pl.ds(NB * y, NB)]

    def gain_copy(n):
        if n == 0:
            return remote(gain_all.at[t], gain_all.at[t], gain_send.at[0], gain_recv.at[0], b=1 - b)
        return remote(gain_pair, gain_pair, gain_send.at[n], gain_recv.at[n], y=lax.rem(y + n, NY))

    def gain_relay():
        other = gain_all.at[NB * y + 1 - b]
        remote(other, other, gain_send.at[0], gain_recv.at[0], b=1 - b).wait_recv()
        for n in range(1, NY):
            gain_copy(n).start()

    def gain_wait():
        for n in range(1, NY):
            pair = gain_all.at[pl.ds(NB * lax.rem(y + NY - n, NY), NB)]
            remote(pair, pair, gain_send.at[n], gain_recv.at[n], y=lax.rem(y + n, NY)).wait_recv()

    def cz_copy(dz):
        to = lax.rem(z + dz, NZ)
        return remote(cot_v.at[:, cot_cols(to)], c_slot(z), cz_send, cz_recv, z=to)

    def cz_start():
        load_cot.wait()
        for dz in range(1, NZ):
            cz_copy(dz).start()

    cz_bulk = cot_v.at[:, pl.ds(0, (NZ - 1) * slab)]

    def cz_wait():
        own_cot.wait()
        wait_bytes(cz_bulk, cz_recv)

    def width(k):
        return 2 if 0 < k < NZ // 2 else 1

    def slot_of(k, j):
        return lax.rem(z + (k if j else NZ - k), NZ)

    def view(buffer, k, *index):
        return buffer.at[(k, *index)] if width(k) == 2 else buffer.at[(k, *index, 0)]

    def rs_copy(k, o):
        to = peer(o)
        piece = part_send.at[k, to["a"], to["y"], to["b"]]
        landing = view(part_recv, k, o)
        return remote(piece if width(k) == 2 else piece.at[0], landing, rs_send.at[k], rs_recv.at[k], **to)

    def rs_bulk(k):
        return view(part_recv, k, pl.ds(1, NP - 1))

    def mid_copies(k):
        copies = []
        for i, offset in enumerate(X_OFFSETS):
            to = peer(OFFSETS.index(offset))
            piece = part_send.at[k, to["a"], :, to["b"], 0]
            copies.append(remote(piece, row_in.at[k, i], mid_send.at[2 * k], mid_recv.at[2 * k], **to))
        for i, offset in enumerate(Y_OFFSETS):
            to = peer(OFFSETS.index(offset))
            for n in range(NA):
                piece = part_send.at[k, n, to["y"], :, 1]
                landing = col_in.at[k, i, n]
                copies.append(remote(piece, landing, mid_send.at[2 * k + 1], mid_recv.at[2 * k + 1], **to))
        return copies

    def last_copies(k):
        copies = []
        for i, offset in enumerate(Y_OFFSETS):
            to = peer(OFFSETS.index(offset))
            piece = row_out.at[k, to["y"]]
            copies.append(remote(piece, row_last.at[k, i], last_send.at[2 * k], last_recv.at[2 * k], **to))
        for i, offset in enumerate(X_OFFSETS):
            to = peer(OFFSETS.index(offset))
            piece = col_out.at[k, to["a"], to["b"]]
            copies.append(remote(piece, col_last.at[k, i], last_send.at[2 * k + 1], last_recv.at[2 * k + 1], **to))
        return copies

    def rs_start(k, paired=False):
        copies = mid_copies(k) if paired else [rs_copy(k, o) for o in range(1, NP)]
        for copy in copies:
            copy.start()

    def rs_mid(k):
        wait_bytes(row_in.at[k], mid_recv.at[2 * k])
        total = part_send[k, a, :, b, 0].astype(F32)
        for i in range(3):
            total = total + row_in[k, i].astype(F32)
        row_out[k] = total.astype(BF16)
        wait_bytes(col_in.at[k], mid_recv.at[2 * k + 1])
        total = part_send[k, :, y, :, 1].astype(F32)
        for i in range(3):
            total = total + col_in[k, i].astype(F32)
        col_out[k] = total.astype(BF16)
        for copy in last_copies(k):
            copy.start()

    def rs_sum(k, paired=False):
        if paired:
            wait_bytes(row_last.at[k], last_recv.at[2 * k])
            total = row_out[k, y].astype(F32)
            for i in range(3):
                total = total + row_last[k, i].astype(F32)
            sums[k, 0] = total.astype(BF16)
            wait_bytes(col_last.at[k], last_recv.at[2 * k + 1])
            total = col_out[k, a, b].astype(F32)
            for i in range(3):
                total = total + col_last[k, i].astype(F32)
            sums[k, 1] = total.astype(BF16)
            return
        wait_bytes(rs_bulk(k), rs_recv.at[k])
        for j in range(width(k)):
            total = part_send[k, a, y, b, j].astype(F32)
            for o in range(1, NP):
                total = total + part_recv[k, o, j].astype(F32)
            sums[k, j] = total.astype(BF16)

    def rs_drain(k, paired=False):
        if paired:
            wait_bytes(row_in.at[k], mid_send.at[2 * k])
            wait_bytes(col_in.at[k], mid_send.at[2 * k + 1])
            wait_bytes(row_last.at[k], last_send.at[2 * k])
            wait_bytes(col_last.at[k], last_send.at[2 * k + 1])
        else:
            wait_bytes(rs_bulk(k), rs_send.at[k])

    def z_copy(k, j):
        return remote(sums.at[k, j], z_in.at[k, width(k) - 1 - j], z_send, z_recv.at[k], z=slot_of(k, j))

    def z_start(k):
        for j in range(width(k)):
            if k:
                z_copy(k, j).start()

    def z_finish(k):
        if k:
            wait_bytes(view(z_in, k), z_recv.at[k])
        for j in range(width(k)):
            index = slot_of(k, j)
            before = x_all[a, index, t // 4, pl.ds(pl.multiple_of(lax.rem(t, 4) * sub, sub), sub), :]
            added = z_in[k, j] if k else sums[k, j]
            whole[k, j] = (before.astype(F32) + added.astype(F32)).astype(BF16)
        ag_start(k)

    def ag_copy(k, o):
        return remote(view(whole, k), view(x1_all, k, place), ag_send.at[k], ag_recv.at[k], section=1, **peer(o))

    def ag_bulk(k):
        return view(x1_all, k, slice(None))

    def ag_start(k):
        for o in range(NP):
            ag_copy(k, o).start()

    def ag_wait(k):
        wait_bytes(ag_bulk(k), ag_recv.at[k])

    def store_part(k, j, which, product):
        part_send[k, :, :, :, j, :, pl.ds(which * cols, cols)] = product.astype(BF16).reshape(NA, NY, NB, sub, cols)

    def down_product(k, j):
        for which in range(NA):
            hidden = h_all[slot_of(k, j)]
            store_part(k, j, which, lax.dot_general(hidden, down_own[which], COL_COL, preferred_element_type=F32))

    def up_start():
        acc_h[...] = jnp.zeros_like(acc_h)
        squares[...] = jnp.zeros_like(squares)

    def up_step(block, index):
        block = block.reshape(NA * rows, slab).astype(F32)
        scaled = (block * gain_all[index]).astype(BF16)
        for which in range(NA):
            acc_h[...] += lax.dot_general(
                scaled[:, which * cols : (which + 1) * cols], up_all[index, which], ROW_ROW, preferred_element_type=F32
            )
        squares[...] += jnp.sum(block * block, axis=1, keepdims=True)

    def finish_hidden():
        inverse_rms = lax.rsqrt(squares[...] * (1.0 / (NT * slab)) + EPS)
        hidden = jax.nn.gelu(acc_h[...] * inverse_rms, approximate=True).astype(BF16)
        h_all[z] = hidden.T

    ahead = lax.rem(t - z + NZ, NZ)
    own_k = jnp.minimum(ahead, NZ - ahead)
    own_j = 1 - jnp.minimum(lax.rem(ahead + NZ - 1, NZ) // 3, 1)
    own_states = x1_all.at[own_k, pl.ds(pl.multiple_of(NT * a, NT), NT), own_j]
    back = remote(own_states, final, back_send, back_recv, section=1 - s)

    def final_copy(k, j):
        return remote(
            sums.at[k, j], final.at[t], f_send.at[min(k, 1)], f_recv, z=slot_of(k, j), y=z // NB, b=lax.rem(z, NB)
        )

    final_local = pltpu.make_async_copy(sums.at[0, 0], final.at[t], f_recv)

    def gradient():
        acc_g[...] = jnp.zeros_like(acc_g)

        @pl.loop(0, NZ)
        def _(index):
            block = c_all[:, index // 4, lax.rem(index, 4)].reshape(NP * sub, slab)
            acc_g[...] += jnp.dot(h_all[index], block, preferred_element_type=F32)

        g_send[...] = acc_g[...].astype(BF16)

    swap = remote(g_send.at[:, their_cols], g_recv, g_ssem, g_rsem, a=other_a)

    @pl.when(first)
    def _():
        for q in range(4):
            bx_copy(q).start()
        for r in range(4):
            own_ring.start(r)
        gain_copy(0).start()
        x_plane.start()
        own_ring.arrive_step(1)
        gain_relay()
        x_plane.relay()
        load_down.wait()
        ex_down.start()
        up_start()
        own_ring.arrive_step(2)
        own_x[0].wait()
        own_x[1].wait()
        gain_wait()
        own_ring.arrive_step(3)
        x_plane.wait()

        def up_slots(k):
            b_wait(k)
            for j in range(width(k)):
                up_step(x_all[:, slot_of(k, j)], slot_of(k, j))

        for k in range(STEPS - 1):
            up_slots(k)
        own_ring.arrive_step(4)
        up_slots(STEPS - 1)
        finish_hidden()
        own_down.wait()
        from_down.wait_recv()
        for r in range(4):
            h_ring.start(r)
        for k in range(STEPS):
            if k:
                h_ring.arrive_step(k)
            if k == GATE_STEP:
                pl.semaphore_signal(gate.at[1], inc=1, device_id={"section": 1 - s}, device_id_type=MESH)
            for j in range(width(k)):
                down_product(k, j)
            rs_start(k, k in PAIRED[0])
            if k - 1 in PAIRED[0]:
                rs_mid(k - 1)
            if k >= 2:
                rs_sum(k - 2, k - 2 in PAIRED[0])
                z_start(k - 2)
            if k >= 3:
                z_finish(k - 3)
        cz_start()
        if STEPS - 2 in PAIRED[0]:
            rs_mid(STEPS - 2)
        rs_sum(STEPS - 2, STEPS - 2 in PAIRED[0])
        z_start(STEPS - 2)
        z_finish(STEPS - 3)
        rs_sum(STEPS - 1)
        z_start(STEPS - 1)
        z_finish(STEPS - 2)
        z_finish(STEPS - 1)
        cz_wait()
        own_c.start()
        c_plane.start()
        c_plane.relay()
        own_c.wait()
        c_plane.wait()
        gradient()
        swap.start()
        back.wait_recv()
        states[...] = final[...].reshape(rows, slab)

    @pl.when(second)
    def _():
        gain_copy(0).start()
        cz_start()
        for q in range(4):
            bx_wait(q)
            b_ring.start(q)
        b_start(0)
        for k in range(1, STEPS):
            b_ring.arrive_step(k)
            b_start(k)
            if k == 1:
                up_start()
                cz_wait()
                own_c.start()
                c_plane.start()
            if k == 2:
                gain_relay()
                load_down.wait()
                ex_up(0).start()
                ex_up(1).start()
                ex_down.start()
            if k == 3:
                c_plane.relay()
        own_down.wait()
        from_up(0).wait_recv()
        from_up(1).wait_recv()
        from_down.wait_recv()
        gain_wait()
        pl.semaphore_wait(gate.at[1], 1)
        for r in range(4):
            up_ring.start(r)

        def up_slots(k):
            ag_wait(k)
            for j in range(width(k)):
                up_step(x1_all[k, :, j], slot_of(k, j))

        up_ring.arrive_step(1)
        up_ring.arrive_step(2)
        up_slots(0)
        up_ring.arrive_step(3)
        up_slots(1)
        up_ring.arrive_step(4)
        up_slots(2)
        up_slots(3)
        up_slots(4)
        finish_hidden()

        def send_home(k):
            rs_sum(k, k in PAIRED[1])
            for j in range(width(k)):
                if k:
                    final_copy(k, j).start()
                else:
                    @pl.when(z == t)
                    def _():
                        final_local.start()

                    @pl.when(z != t)
                    def _():
                        final_copy(0, 0).start()

        for r in range(4):
            h_ring.start(r)
        back.start()
        for k in range(STEPS):
            if k:
                h_ring.arrive_step(k)
            for j in range(width(k)):
                down_product(k, j)
            rs_start(k, k in PAIRED[1])
            if k - 1 in PAIRED[1]:
                rs_mid(k - 1)
            if k >= 2:
                send_home(k - 2)

        own_c.wait()
        c_plane.wait()
        gradient()
        swap.start()
        for k in (STEPS - 2, STEPS - 1):
            send_home(k)
        wait_bytes(final, f_recv)
        own_rows = x1_all[own_k, pl.ds(pl.multiple_of(NT * a, NT), NT), own_j].astype(F32)
        states[...] = (own_rows + final[...].astype(F32)).astype(BF16).reshape(rows, slab)

    grad[my_rows, :] = g_send[:, my_cols]
    swap.wait_recv()
    grad[their_rows, :] = g_recv[...]

    swap.wait_send()
    ex_down.wait_send()
    for n in range(NY):
        gain_copy(n).wait_send()
    wait_bytes(cz_bulk, cz_send)
    c_plane.drain()
    own_ring.drain()
    h_ring.drain()

    @pl.when(first)
    def _():
        x_plane.drain()
        for k in range(STEPS):
            rs_drain(k, k in PAIRED[0])
        wait_bytes(up_b.at[0], bx_send)
        wait_bytes(final.at[pl.ds(0, NZ - 1)], z_send)
        for k in range(STEPS):
            wait_bytes(ag_bulk(k), ag_send.at[k])

    @pl.when(second)
    def _():
        back.wait_send()
        for k in range(STEPS):
            rs_drain(k, k in PAIRED[1])
        up_ring.drain()
        ex_up(0).wait_send()
        ex_up(1).wait_send()
        wait_bytes(up_b, b_send)
        wait_bytes(final.at[pl.ds(0, NZ - 1)], f_send.at[1])

        @pl.when(z != t)
        def _():
            final_copy(0, 0).wait_send()


def body(tokens, gain, w_up, w_down, cotangent):
    rows, slab = tokens.shape
    cols, hidden = w_up.shape[1:]
    half = hidden // 2
    sub = rows // NT
    dma = pltpu.SemaphoreType.DMA
    vmem = pl.BlockSpec(memory_space=pltpu.VMEM)
    states, grad = pl.pallas_call(
        kernel,
        out_shape=(
            jax.ShapeDtypeStruct((rows, slab), BF16),
            jax.ShapeDtypeStruct((hidden, cols), BF16),
        ),
        in_specs=[pl.BlockSpec(memory_space=pltpu.HBM)] * 5,
        out_specs=(vmem, vmem),
        scratch_shapes=[
            pltpu.VMEM((rows, slab), BF16),
            pltpu.VMEM((1, slab), BF16),
            pltpu.VMEM((cols, hidden), BF16),
            pltpu.VMEM((hidden, cols), BF16),
            pltpu.VMEM((half, cols), BF16),
            pltpu.VMEM((sub, NT * slab), BF16),
            pltpu.VMEM((NA * rows, 1), F32),
            pltpu.VMEM((NZ, NA, half, cols), BF16),
            pltpu.VMEM((NZ, half, cols), BF16),
            pltpu.VMEM((NA, half, cols), BF16),
            pltpu.VMEM((NA, NT, 2, rows // 2, slab), BF16),
            pltpu.VMEM((STEPS, NP, 2, sub, slab), BF16),
            pltpu.VMEM((NZ, half, NA * rows), BF16),
            pltpu.VMEM((2, NZ // 2, sub, slab), BF16),
            pltpu.VMEM((NP, 2, NZ // 2, sub, slab), BF16),
            pltpu.VMEM((NT, 1, slab), F32),
            pltpu.VMEM((STEPS, NA, NY, NB, 2, sub, slab), BF16),
            pltpu.VMEM((STEPS, NP, 2, sub, slab), BF16),
            pltpu.VMEM((STEPS, 3, NY, sub, slab), BF16),
            pltpu.VMEM((STEPS, 3, NA, NB, sub, slab), BF16),
            pltpu.VMEM((STEPS, NY, sub, slab), BF16),
            pltpu.VMEM((STEPS, NA, NB, sub, slab), BF16),
            pltpu.VMEM((STEPS, 3, sub, slab), BF16),
            pltpu.VMEM((STEPS, 3, sub, slab), BF16),
            pltpu.VMEM((STEPS, 2, sub, slab), BF16),
            pltpu.VMEM((STEPS, 2, sub, slab), BF16),
            pltpu.VMEM((STEPS, 2, sub, slab), BF16),
            pltpu.VMEM((NT, sub, slab), BF16),
            pltpu.VMEM((NA * rows, half), F32),
            pltpu.VMEM((half, NA * cols), F32),
            pltpu.VMEM((half, NA * cols), BF16),
            pltpu.VMEM((half, cols), BF16),
            dma((3,)), dma((3,)), dma, dma((4,)), dma, dma((STEPS,)), dma, dma((STEPS,)), dma((10,)), dma((NY,)), dma((NY,)),
            dma((STEPS,)), dma((STEPS,)), dma((2 * STEPS,)), dma((2 * STEPS,)), dma((2 * STEPS,)), dma((2 * STEPS,)),
            dma((STEPS,)), dma((STEPS,)),
            dma((2,)), dma, dma, dma, dma, dma, dma, dma,
        ]
        + [dma, dma((Ring.COUNT,)), dma, dma((Ring.COUNT,))] * 3
        + [dma, dma((6,)), dma, dma] * 2
        + [pltpu.SemaphoreType.REGULAR((2,))],
        compiler_params=pltpu.CompilerParams(
            collective_id=0, has_side_effects=True, vmem_limit_bytes=48 * 1024 * 1024
        ),
    )(*[pltpu.with_memory_space_constraint(x, pltpu.HBM) for x in (tokens, gain, w_up[0], w_down[0], cotangent[0])])
    return states[None], grad[None]


def solution(mesh):
    torus = Mesh(
        mesh.devices.reshape(mesh.shape["section"], NZ, NA, NY, NB), ("section", "z", "a", "y", "b")
    )
    dp, tensor = ("z", "a"), ("y", "b")
    in_specs = (
        P(dp, tensor),
        P("section", tensor),
        P("section", dp, tensor),
        P("section", tensor, dp),
        P("section", dp, None),
    )
    out_specs = (P("section", dp, tensor), P("section", tensor, dp))
    return jax.shard_map(body, mesh=torus, in_specs=in_specs, out_specs=out_specs, check_vma=False)
```

```python
import jax
import jax.numpy as jnp
from jax import lax
from jax.experimental import pallas as pl
from jax.experimental.pallas import tpu as pltpu
from jax.sharding import Mesh
from jax.sharding import PartitionSpec as P

NZ, NA, NY, NB = 8, 2, 4, 2
NT = NY * NB
NP = NA * NT
STEPS = NZ // 2 + 1
GATE_STEP = 2
PAIRED = ((), (2, 3))
EPS = 1e-06
MESH = pl.DeviceIdType.MESH
F32 = jnp.float32
BF16 = jnp.bfloat16
OFFSETS = [(da, dy, db) for da in range(NA) for dy in range(NY) for db in range(NB)]
X_OFFSETS = [(1, 0, 0), (0, 0, 1), (1, 0, 1)]
Y_OFFSETS = [(0, dy, 0) for dy in range(1, NY)]
ROW_ROW = (((1,), (1,)), ((), ()))
COL_COL = (((0,), (0,)), ((), ()))


def remote(src, dst, send, recv, **where):
    return pltpu.make_async_remote_copy(
        src_ref=src, dst_ref=dst, send_sem=send, recv_sem=recv, device_id=where, device_id_type=MESH
    )


def wait_bytes(like, sem):
    pltpu.make_async_copy(like, like, sem).wait()


class Ring:
    COUNT = 14
    STEPS = ((0, 1, 2, 3), (4, 5, 6, 7), (8, 9, 10, 11), (12, 13))
    LEAD_STEPS = ((0, 1, 4, 5, 2, 3), (8, 9, 6, 7), (12, 10, 11), (13,))

    def __init__(self, z, piece, bulk, sems, steps=STEPS):
        self.z, self.piece, self.bulk, self.steps = z, piece, bulk, steps
        self.right_send, self.right_recv, self.left_send, self.left_recv = sems

    def _copy(self, origin, q, to_right, r):
        piece = self.piece(lax.rem(origin, NZ), q)
        if to_right:
            return remote(piece, piece, self.right_send, self.right_recv.at[r], z=lax.rem(self.z + 1, NZ))
        return remote(piece, piece, self.left_send, self.left_recv.at[r], z=lax.rem(self.z + NZ - 1, NZ))

    def _q(self, r, to_right):
        if r < 12:
            return r % 4
        return 2 * (r - 12) + (0 if to_right else 1)

    def right(self, r):
        return self._copy(self.z + NZ - r // 4, self._q(r, True), True, r)

    def left(self, r):
        return self._copy(self.z + r // 4, self._q(r, False), False, r)

    def start(self, r):
        self.right(r).start()
        self.left(r).start()

    def arrive(self, r):
        self._copy(self.z + 2 * NZ - 1 - r // 4, self._q(r, True), True, r).wait_recv()
        if r < 8:
            self.right(r + 4).start()
        elif r in (8, 10):
            self.right(12 + (r - 8) // 2).start()
        self._copy(self.z + 1 + r // 4, self._q(r, False), False, r).wait_recv()
        if r < 8:
            self.left(r + 4).start()
        elif r in (9, 11):
            self.left(12 + (r - 9) // 2).start()

    def arrive_step(self, k):
        for r in self.steps[k - 1]:
            self.arrive(r)

    def drain(self):
        wait_bytes(self.bulk, self.right_send)
        wait_bytes(self.bulk, self.left_send)


class Plane:
    def __init__(self, me, own, slot, bulk, sems):
        self.me, self.own, self.slot, self.bulk = me, own, slot, bulk
        self.send1, self.recv1, self.send2, self.recv2 = sems

    def _at(self, *offsets):
        a, y, b = self.me
        for da, dy, db in offsets:
            a, y, b = lax.rem(a + NA - da, NA), lax.rem(y + NY - dy, NY), lax.rem(b + NB - db, NB)
        return a, y, b

    def _peer(self, offset):
        a, y, b = self.me
        da, dy, db = offset
        return {"a": lax.rem(a + da, NA), "y": lax.rem(y + dy, NY), "b": lax.rem(b + db, NB)}

    def _first(self, half, i, origin):
        offset = (X_OFFSETS, Y_OFFSETS)[half][i]
        n = 3 * half + i
        return remote(self.own(half), self.slot(origin, half), self.send1, self.recv1.at[n], **self._peer(offset))

    def _second(self, half, i, piece, origin):
        offset = (Y_OFFSETS, X_OFFSETS)[half][i]
        return remote(piece, self.slot(origin, half), self.send2, self.recv2, **self._peer(offset))

    def start(self):
        for half in (0, 1):
            for i in range(3):
                self._first(half, i, self.me).start()
        for half in (0, 1):
            for i in range(3):
                self._second(half, i, self.own(half), self.me).start()

    def relay(self):
        for i in range(3):
            for half in (0, 1):
                origin = self._at((X_OFFSETS, Y_OFFSETS)[half][i])
                self._first(half, i, origin).wait_recv()
                piece = self.slot(origin, half)
                for n in range(3):
                    self._second(half, n, piece, origin).start()

    def wait(self):
        wait_bytes(self.bulk(24), self.recv2)

    def drain(self):
        wait_bytes(self.bulk(6), self.send1)
        wait_bytes(self.bulk(24), self.send2)


def kernel(
    tokens, gain, w_up, down, cot, states, grad,
    tok_v, gain_v, w_v, up_t, down_v, cot_v, squares,
    up_all, up_b, down_own, x_all, x1_all, h_all, c_z, c_all, gain_all, part_send, part_recv, row_in, col_in, row_out, col_out, row_last, col_last, sums, z_in, whole, final,
    acc_h, acc_g, g_send, g_recv,
    ex_send, ex_recv, bx_send, bx_recv, b_send, b_recv, z_send, z_recv, own_sem, gain_send, gain_recv, rs_send, rs_recv, mid_send, mid_recv, last_send, last_recv, ag_send, ag_recv, f_send, f_recv,
    cz_send, cz_recv, back_send, back_recv, g_ssem, g_rsem,
    u0, u1, u2, u3, a0, a1, a2, a3, h0, h1, h2, h3, x0, x1, x2, x3, c0, c1, c2, c3, gate,
):
    s = lax.axis_index("section")
    z = lax.axis_index("z")
    a = lax.axis_index("a")
    y = lax.axis_index("y")
    b = lax.axis_index("b")
    t = y * NB + b
    place = a * NT + t
    me = (a, y, b)
    first = s == 0
    second = s == 1
    half = w_up.shape[1] // 2
    cols = w_up.shape[0]
    rows, slab = tokens.shape
    sub = rows // NT
    other_a = 1 - a

    def peer(o):
        da, dy, db = OFFSETS[o]
        return {"a": lax.rem(a + da, NA), "y": lax.rem(y + dy, NY), "b": lax.rem(b + db, NB)}

    def source(o):
        da, dy, db = OFFSETS[o]
        return lax.rem(a + NA - da, NA), lax.rem(y + NY - dy, NY), lax.rem(b + NB - db, NB)

    my_rows = pl.ds(pl.multiple_of(half * a, half), half)
    their_rows = pl.ds(pl.multiple_of(half * other_a, half), half)
    my_cols = pl.ds(pl.multiple_of(cols * a, cols), cols)
    their_cols = pl.ds(pl.multiple_of(cols * other_a, cols), cols)
    cot_rows = pl.ds(pl.multiple_of(sub * t, sub), sub)

    def cot_cols(index):
        return pl.ds(pl.multiple_of(slab * index, slab), slab)

    def c_slot(index):
        return c_z.at[index // 4, lax.rem(index, 4)]

    load_w = pltpu.make_async_copy(w_up, w_v, own_sem.at[0])
    load_tok = pltpu.make_async_copy(tokens, tok_v, own_sem.at[1])
    own_x = [
        pltpu.make_async_copy(tokens.at[pl.ds(rows // 2 * i, rows // 2), :], x_all.at[a, t, i], own_sem.at[2 + i])
        for i in (0, 1)
    ]
    load_gain = pltpu.make_async_copy(gain, gain_v, own_sem.at[4])
    load_down = pltpu.make_async_copy(down.at[their_rows, :], down_v, own_sem.at[5])
    own_down = pltpu.make_async_copy(down.at[my_rows, :], down_own.at[a], own_sem.at[6])
    load_cot = pltpu.make_async_copy(cot.at[cot_rows, :], cot_v, own_sem.at[7])
    own_cot = pltpu.make_async_copy(cot.at[cot_rows, cot_cols(z)], c_slot(z), own_sem.at[8])
    own_c = pltpu.make_async_copy(c_z, c_all.at[place], own_sem.at[9])
    load_w.start()

    @pl.when(first)
    def _():
        load_tok.start()

    barrier = pltpu.get_barrier_semaphore()
    for dz in range(1, NZ):
        pl.semaphore_signal(barrier, inc=1, device_id={"z": lax.rem(z + dz, NZ)}, device_id_type=MESH)
    for offset in X_OFFSETS + Y_OFFSETS:
        pl.semaphore_signal(barrier, inc=1, device_id=peer(OFFSETS.index(offset)), device_id_type=MESH)
    pl.semaphore_signal(barrier, inc=1, device_id={"section": 1 - s}, device_id_type=MESH)

    @pl.when(second)
    def _():
        pl.semaphore_signal(barrier, inc=1, device_id={"section": 0, "a": other_a}, device_id_type=MESH)

    @pl.when(first)
    def _():
        own_x[0].start()
        own_x[1].start()

    load_gain.start()
    load_down.start()
    own_down.start()
    load_cot.start()
    own_cot.start()
    load_w.wait()
    up_t[...] = w_v[...].T
    up_all[z, a] = up_t[my_rows, :]
    load_gain.wait()
    gain_all[t] = gain_v[...].astype(F32)

    @pl.when(first)
    def _():
        load_tok.wait()

    greeted = NZ - 1 + len(X_OFFSETS) + len(Y_OFFSETS) + 1

    @pl.when(first)
    def _():
        pl.semaphore_wait(barrier, greeted + 1)

    @pl.when(second)
    def _():
        pl.semaphore_wait(barrier, greeted)

    quarter_rows = half // 2

    def ex_up(i):
        rows_there = pl.ds(pl.multiple_of(half * other_a + quarter_rows * i, quarter_rows), quarter_rows)
        landing = up_all.at[z, a, pl.ds(quarter_rows * i, quarter_rows), :]
        return remote(up_t.at[rows_there, :], landing, ex_send.at[i], ex_recv.at[i], a=other_a)

    def from_up(i):
        landing = up_all.at[z, other_a, pl.ds(quarter_rows * i, quarter_rows), :]
        return remote(landing, landing, ex_send.at[i], ex_recv.at[i], a=other_a)

    ex_down = remote(down_v, down_own.at[a], ex_send.at[2], ex_recv.at[2], a=other_a)
    from_down = remote(down_v, down_own.at[other_a], ex_send.at[2], ex_recv.at[2], a=other_a)

    b_rows = half // 4

    def bx_copy(q):
        rows_there = pl.ds(pl.multiple_of(half * other_a + b_rows * q, b_rows), b_rows)
        landing = up_b.at[z, pl.ds(b_rows * q, b_rows), :]
        return remote(up_t.at[rows_there, :], landing, bx_send, bx_recv.at[q], a=other_a, section=1)

    def bx_wait(q):
        landing = up_b.at[z, pl.ds(b_rows * q, b_rows), :]
        pltpu.make_async_copy(landing, landing, bx_recv.at[q]).wait()

    def b_copy(k, j):
        slot = lax.rem(z + (k if j else NZ - k), NZ)
        return remote(up_b.at[slot], up_all.at[slot, other_a], b_send, b_recv.at[k], section=0)

    def b_start(k):
        for j in range(2 if 0 < k < NZ // 2 else 1):
            b_copy(k, j).start()

    def b_wait(k):
        wait_bytes(up_b.at[pl.ds(0, 2 if 0 < k < NZ // 2 else 1)], b_recv.at[k])


    def quarter(buffer):
        def piece(origin, q):
            which = a if q < 2 else other_a
            return buffer.at[origin, which, pl.ds(q % 2 * quarter_rows, quarter_rows), :]

        return piece

    up_ring = Ring(z, quarter(up_all), up_all.at[pl.ds(0, 7), 0], (u0, u1, u2, u3), Ring.LEAD_STEPS)
    own_ring = Ring(
        z,
        lambda origin, q: up_all.at[origin, a, pl.ds(q * b_rows, b_rows), :],
        up_b.at[pl.ds(0, 7), pl.ds(0, 2 * b_rows), :],
        (a0, a1, a2, a3),
    )
    b_ring = Ring(
        z,
        lambda origin, q: up_b.at[origin, pl.ds(q * b_rows, b_rows), :],
        up_b.at[pl.ds(0, 7), pl.ds(0, 2 * b_rows), :],
        (a0, a1, a2, a3),
    )
    h_rows = half // 4
    h_ring = Ring(
        z,
        lambda origin, q: h_all.at[origin, pl.ds(q * h_rows, h_rows), :],
        h_all.at[pl.ds(0, 7), pl.ds(0, 2 * h_rows), :],
        (h0, h1, h2, h3),
    )
    x_plane = Plane(
        me,
        lambda i: tok_v.at[pl.ds(rows // 2 * i, rows // 2), :],
        lambda at, i: x_all.at[at[0], at[1] * NB + at[2], i],
        lambda n: x_all.at[:, pl.ds(0, n // 4)] if n == 24 else x_all.at[0, pl.ds(0, n // 2)],
        (x0, x1, x2, x3),
    )
    c_plane = Plane(
        me,
        lambda i: c_z.at[i],
        lambda at, i: c_all.at[at[0] * NT + at[1] * NB + at[2], i],
        lambda n: c_all.at[pl.ds(0, n // 2)],
        (c0, c1, c2, c3),
    )

    gain_pair = gain_all.at[pl.ds(NB * y, NB)]

    def gain_copy(n):
        if n == 0:
            return remote(gain_all.at[t], gain_all.at[t], gain_send.at[0], gain_recv.at[0], b=1 - b)
        return remote(gain_pair, gain_pair, gain_send.at[n], gain_recv.at[n], y=lax.rem(y + n, NY))

    def gain_relay():
        other = gain_all.at[NB * y + 1 - b]
        remote(other, other, gain_send.at[0], gain_recv.at[0], b=1 - b).wait_recv()
        for n in range(1, NY):
            gain_copy(n).start()

    def gain_wait():
        for n in range(1, NY):
            pair = gain_all.at[pl.ds(NB * lax.rem(y + NY - n, NY), NB)]
            remote(pair, pair, gain_send.at[n], gain_recv.at[n], y=lax.rem(y + n, NY)).wait_recv()

    def cz_copy(dz):
        to = lax.rem(z + dz, NZ)
        return remote(cot_v.at[:, cot_cols(to)], c_slot(z), cz_send, cz_recv, z=to)

    def cz_start():
        load_cot.wait()
        for dz in range(1, NZ):
            cz_copy(dz).start()

    cz_bulk = cot_v.at[:, pl.ds(0, (NZ - 1) * slab)]

    def cz_wait():
        own_cot.wait()
        wait_bytes(cz_bulk, cz_recv)

    def width(k):
        return 2 if 0 < k < NZ // 2 else 1

    def slot_of(k, j):
        return lax.rem(z + (k if j else NZ - k), NZ)

    def view(buffer, k, *index):
        return buffer.at[(k, *index)] if width(k) == 2 else buffer.at[(k, *index, 0)]

    def rs_copy(k, o):
        to = peer(o)
        piece = part_send.at[k, to["a"], to["y"], to["b"]]
        landing = view(part_recv, k, o)
        return remote(piece if width(k) == 2 else piece.at[0], landing, rs_send.at[k], rs_recv.at[k], **to)

    def rs_bulk(k):
        return view(part_recv, k, pl.ds(1, NP - 1))

    def mid_copies(k):
        copies = []
        for i, offset in enumerate(X_OFFSETS):
            to = peer(OFFSETS.index(offset))
            piece = part_send.at[k, to["a"], :, to["b"], 0]
            copies.append(remote(piece, row_in.at[k, i], mid_send.at[2 * k], mid_recv.at[2 * k], **to))
        for i, offset in enumerate(Y_OFFSETS):
            to = peer(OFFSETS.index(offset))
            for n in range(NA):
                piece = part_send.at[k, n, to["y"], :, 1]
                landing = col_in.at[k, i, n]
                copies.append(remote(piece, landing, mid_send.at[2 * k + 1], mid_recv.at[2 * k + 1], **to))
        return copies

    def last_copies(k):
        copies = []
        for i, offset in enumerate(Y_OFFSETS):
            to = peer(OFFSETS.index(offset))
            piece = row_out.at[k, to["y"]]
            copies.append(remote(piece, row_last.at[k, i], last_send.at[2 * k], last_recv.at[2 * k], **to))
        for i, offset in enumerate(X_OFFSETS):
            to = peer(OFFSETS.index(offset))
            piece = col_out.at[k, to["a"], to["b"]]
            copies.append(remote(piece, col_last.at[k, i], last_send.at[2 * k + 1], last_recv.at[2 * k + 1], **to))
        return copies

    def rs_start(k, paired=False):
        copies = mid_copies(k) if paired else [rs_copy(k, o) for o in range(1, NP)]
        for copy in copies:
            copy.start()

    def rs_mid(k):
        wait_bytes(row_in.at[k], mid_recv.at[2 * k])
        total = part_send[k, a, :, b, 0].astype(F32)
        for i in range(3):
            total = total + row_in[k, i].astype(F32)
        row_out[k] = total.astype(BF16)
        wait_bytes(col_in.at[k], mid_recv.at[2 * k + 1])
        total = part_send[k, :, y, :, 1].astype(F32)
        for i in range(3):
            total = total + col_in[k, i].astype(F32)
        col_out[k] = total.astype(BF16)
        for copy in last_copies(k):
            copy.start()

    def rs_sum(k, paired=False):
        if paired:
            wait_bytes(row_last.at[k], last_recv.at[2 * k])
            total = row_out[k, y].astype(F32)
            for i in range(3):
                total = total + row_last[k, i].astype(F32)
            sums[k, 0] = total.astype(BF16)
            wait_bytes(col_last.at[k], last_recv.at[2 * k + 1])
            total = col_out[k, a, b].astype(F32)
            for i in range(3):
                total = total + col_last[k, i].astype(F32)
            sums[k, 1] = total.astype(BF16)
            return
        wait_bytes(rs_bulk(k), rs_recv.at[k])
        for j in range(width(k)):
            total = part_send[k, a, y, b, j].astype(F32)
            for o in range(1, NP):
                total = total + part_recv[k, o, j].astype(F32)
            sums[k, j] = total.astype(BF16)

    def rs_drain(k, paired=False):
        if paired:
            wait_bytes(row_in.at[k], mid_send.at[2 * k])
            wait_bytes(col_in.at[k], mid_send.at[2 * k + 1])
            wait_bytes(row_last.at[k], last_send.at[2 * k])
            wait_bytes(col_last.at[k], last_send.at[2 * k + 1])
        else:
            wait_bytes(rs_bulk(k), rs_send.at[k])

    def z_copy(k, j):
        return remote(sums.at[k, j], z_in.at[k, width(k) - 1 - j], z_send, z_recv.at[k], z=slot_of(k, j))

    def z_start(k):
        for j in range(width(k)):
            if k:
                z_copy(k, j).start()

    def z_finish(k):
        if k:
            wait_bytes(view(z_in, k), z_recv.at[k])
        for j in range(width(k)):
            index = slot_of(k, j)
            before = x_all[a, index, t // 4, pl.ds(pl.multiple_of(lax.rem(t, 4) * sub, sub), sub), :]
            added = z_in[k, j] if k else sums[k, j]
            whole[k, j] = (before.astype(F32) + added.astype(F32)).astype(BF16)
        ag_start(k)

    def ag_copy(k, o):
        return remote(view(whole, k), view(x1_all, k, place), ag_send.at[k], ag_recv.at[k], section=1, **peer(o))

    def ag_bulk(k):
        return view(x1_all, k, slice(None))

    def ag_start(k):
        for o in range(NP):
            ag_copy(k, o).start()

    def ag_wait(k):
        wait_bytes(ag_bulk(k), ag_recv.at[k])

    def store_part(k, j, which, product):
        part_send[k, :, :, :, j, :, pl.ds(which * cols, cols)] = product.astype(BF16).reshape(NA, NY, NB, sub, cols)

    def down_product(k, j):
        for which in range(NA):
            hidden = h_all[slot_of(k, j)]
            store_part(k, j, which, lax.dot_general(hidden, down_own[which], COL_COL, preferred_element_type=F32))

    def up_start():
        acc_h[...] = jnp.zeros_like(acc_h)
        squares[...] = jnp.zeros_like(squares)

    def up_step(block, index):
        block = block.reshape(NA * rows, slab).astype(F32)
        scaled = (block * gain_all[index]).astype(BF16)
        for which in range(NA):
            acc_h[...] += lax.dot_general(
                scaled[:, which * cols : (which + 1) * cols], up_all[index, which], ROW_ROW, preferred_element_type=F32
            )
        squares[...] += jnp.sum(block * block, axis=1, keepdims=True)

    def finish_hidden():
        inverse_rms = lax.rsqrt(squares[...] * (1.0 / (NT * slab)) + EPS)
        hidden = jax.nn.gelu(acc_h[...] * inverse_rms, approximate=True).astype(BF16)
        h_all[z] = hidden.T

    ahead = lax.rem(t - z + NZ, NZ)
    own_k = jnp.minimum(ahead, NZ - ahead)
    own_j = 1 - jnp.minimum(lax.rem(ahead + NZ - 1, NZ) // 3, 1)
    own_states = x1_all.at[own_k, pl.ds(pl.multiple_of(NT * a, NT), NT), own_j]
    back = remote(own_states, final, back_send, back_recv, section=1 - s)

    def final_copy(k, j):
        return remote(
            sums.at[k, j], final.at[t], f_send.at[min(k, 1)], f_recv, z=slot_of(k, j), y=z // NB, b=lax.rem(z, NB)
        )

    final_local = pltpu.make_async_copy(sums.at[0, 0], final.at[t], f_recv)

    def gradient():
        acc_g[...] = jnp.zeros_like(acc_g)

        @pl.loop(0, NZ)
        def _(index):
            block = c_all[:, index // 4, lax.rem(index, 4)].reshape(NP * sub, slab)
            acc_g[...] += jnp.dot(h_all[index], block, preferred_element_type=F32)

        g_send[...] = acc_g[...].astype(BF16)

    swap = remote(g_send.at[:, their_cols], g_recv, g_ssem, g_rsem, a=other_a)

    def write_gradient():
        grad[my_rows, :] = g_send[:, my_cols]
        swap.wait_recv()
        grad[their_rows, :] = g_recv[...]

    @pl.when(first)
    def _():
        for q in range(4):
            bx_copy(q).start()
        for r in range(4):
            own_ring.start(r)
        gain_copy(0).start()
        x_plane.start()
        own_ring.arrive_step(1)
        gain_relay()
        x_plane.relay()
        load_down.wait()
        ex_down.start()
        up_start()
        own_ring.arrive_step(2)
        own_x[0].wait()
        own_x[1].wait()
        gain_wait()
        own_ring.arrive_step(3)
        x_plane.wait()

        def up_slots(k):
            b_wait(k)
            for j in range(width(k)):
                up_step(x_all[:, slot_of(k, j)], slot_of(k, j))

        for k in range(STEPS - 1):
            up_slots(k)
        own_ring.arrive_step(4)
        up_slots(STEPS - 1)
        finish_hidden()
        own_down.wait()
        from_down.wait_recv()
        for r in range(4):
            h_ring.start(r)
        for k in range(STEPS):
            if k:
                h_ring.arrive_step(k)
            if k == GATE_STEP:
                pl.semaphore_signal(gate.at[1], inc=1, device_id={"section": 1 - s}, device_id_type=MESH)
            for j in range(width(k)):
                down_product(k, j)
            rs_start(k, k in PAIRED[0])
            if k - 1 in PAIRED[0]:
                rs_mid(k - 1)
            if k >= 2:
                rs_sum(k - 2, k - 2 in PAIRED[0])
                z_start(k - 2)
            if k >= 3:
                z_finish(k - 3)
        cz_start()
        if STEPS - 2 in PAIRED[0]:
            rs_mid(STEPS - 2)
        rs_sum(STEPS - 2, STEPS - 2 in PAIRED[0])
        z_start(STEPS - 2)
        z_finish(STEPS - 3)
        rs_sum(STEPS - 1)
        z_start(STEPS - 1)
        z_finish(STEPS - 2)
        z_finish(STEPS - 1)
        cz_wait()
        own_c.start()
        c_plane.start()
        c_plane.relay()
        own_c.wait()
        c_plane.wait()
        gradient()
        swap.start()
        back.wait_recv()
        states[...] = final[...].reshape(rows, slab)
        write_gradient()

    @pl.when(second)
    def _():
        gain_copy(0).start()
        cz_start()
        for q in range(4):
            bx_wait(q)
            b_ring.start(q)
        b_start(0)
        for k in range(1, STEPS):
            b_ring.arrive_step(k)
            b_start(k)
            if k == 1:
                up_start()
                cz_wait()
                own_c.start()
                c_plane.start()
            if k == 2:
                gain_relay()
                load_down.wait()
                ex_up(0).start()
                ex_up(1).start()
                ex_down.start()
            if k == 3:
                c_plane.relay()
        own_down.wait()
        from_up(0).wait_recv()
        from_up(1).wait_recv()
        from_down.wait_recv()
        gain_wait()
        pl.semaphore_wait(gate.at[1], 1)
        for r in range(4):
            up_ring.start(r)

        def up_slots(k):
            ag_wait(k)
            for j in range(width(k)):
                up_step(x1_all[k, :, j], slot_of(k, j))

        up_ring.arrive_step(1)
        up_ring.arrive_step(2)
        up_slots(0)
        up_ring.arrive_step(3)
        up_slots(1)
        up_ring.arrive_step(4)
        up_slots(2)
        up_slots(3)
        up_slots(4)
        finish_hidden()

        def send_home(k):
            rs_sum(k, k in PAIRED[1])
            for j in range(width(k)):
                if k:
                    final_copy(k, j).start()
                else:
                    @pl.when(z == t)
                    def _():
                        final_local.start()

                    @pl.when(z != t)
                    def _():
                        final_copy(0, 0).start()

        for r in range(4):
            h_ring.start(r)
        back.start()
        for k in range(STEPS):
            if k:
                h_ring.arrive_step(k)
            for j in range(width(k)):
                down_product(k, j)
            rs_start(k, k in PAIRED[1])
            if k - 1 in PAIRED[1]:
                rs_mid(k - 1)
            if k >= 2:
                send_home(k - 2)

        own_c.wait()
        c_plane.wait()
        gradient()
        swap.start()
        for k in (STEPS - 2, STEPS - 1):
            send_home(k)
        write_gradient()
        wait_bytes(final, f_recv)
        own_rows = x1_all[own_k, pl.ds(pl.multiple_of(NT * a, NT), NT), own_j].astype(F32)
        states[...] = (own_rows + final[...].astype(F32)).astype(BF16).reshape(rows, slab)

    swap.wait_send()
    ex_down.wait_send()
    for n in range(NY):
        gain_copy(n).wait_send()
    wait_bytes(cz_bulk, cz_send)
    c_plane.drain()
    own_ring.drain()
    h_ring.drain()

    @pl.when(first)
    def _():
        x_plane.drain()
        for k in range(STEPS):
            rs_drain(k, k in PAIRED[0])
        wait_bytes(up_b.at[0], bx_send)
        wait_bytes(final.at[pl.ds(0, NZ - 1)], z_send)
        for k in range(STEPS):
            wait_bytes(ag_bulk(k), ag_send.at[k])

    @pl.when(second)
    def _():
        back.wait_send()
        for k in range(STEPS):
            rs_drain(k, k in PAIRED[1])
        up_ring.drain()
        ex_up(0).wait_send()
        ex_up(1).wait_send()
        wait_bytes(up_b, b_send)
        wait_bytes(final.at[pl.ds(0, NZ - 1)], f_send.at[1])

        @pl.when(z != t)
        def _():
            final_copy(0, 0).wait_send()


def body(tokens, gain, w_up, w_down, cotangent):
    rows, slab = tokens.shape
    cols, hidden = w_up.shape[1:]
    half = hidden // 2
    sub = rows // NT
    dma = pltpu.SemaphoreType.DMA
    vmem = pl.BlockSpec(memory_space=pltpu.VMEM)
    states, grad = pl.pallas_call(
        kernel,
        out_shape=(
            jax.ShapeDtypeStruct((rows, slab), BF16),
            jax.ShapeDtypeStruct((hidden, cols), BF16),
        ),
        in_specs=[pl.BlockSpec(memory_space=pltpu.HBM)] * 5,
        out_specs=(vmem, vmem),
        scratch_shapes=[
            pltpu.VMEM((rows, slab), BF16),
            pltpu.VMEM((1, slab), BF16),
            pltpu.VMEM((cols, hidden), BF16),
            pltpu.VMEM((hidden, cols), BF16),
            pltpu.VMEM((half, cols), BF16),
            pltpu.VMEM((sub, NT * slab), BF16),
            pltpu.VMEM((NA * rows, 1), F32),
            pltpu.VMEM((NZ, NA, half, cols), BF16),
            pltpu.VMEM((NZ, half, cols), BF16),
            pltpu.VMEM((NA, half, cols), BF16),
            pltpu.VMEM((NA, NT, 2, rows // 2, slab), BF16),
            pltpu.VMEM((STEPS, NP, 2, sub, slab), BF16),
            pltpu.VMEM((NZ, half, NA * rows), BF16),
            pltpu.VMEM((2, NZ // 2, sub, slab), BF16),
            pltpu.VMEM((NP, 2, NZ // 2, sub, slab), BF16),
            pltpu.VMEM((NT, 1, slab), F32),
            pltpu.VMEM((STEPS, NA, NY, NB, 2, sub, slab), BF16),
            pltpu.VMEM((STEPS, NP, 2, sub, slab), BF16),
            pltpu.VMEM((STEPS, 3, NY, sub, slab), BF16),
            pltpu.VMEM((STEPS, 3, NA, NB, sub, slab), BF16),
            pltpu.VMEM((STEPS, NY, sub, slab), BF16),
            pltpu.VMEM((STEPS, NA, NB, sub, slab), BF16),
            pltpu.VMEM((STEPS, 3, sub, slab), BF16),
            pltpu.VMEM((STEPS, 3, sub, slab), BF16),
            pltpu.VMEM((STEPS, 2, sub, slab), BF16),
            pltpu.VMEM((STEPS, 2, sub, slab), BF16),
            pltpu.VMEM((STEPS, 2, sub, slab), BF16),
            pltpu.VMEM((NT, sub, slab), BF16),
            pltpu.VMEM((NA * rows, half), F32),
            pltpu.VMEM((half, NA * cols), F32),
            pltpu.VMEM((half, NA * cols), BF16),
            pltpu.VMEM((half, cols), BF16),
            dma((3,)), dma((3,)), dma, dma((4,)), dma, dma((STEPS,)), dma, dma((STEPS,)), dma((10,)), dma((NY,)), dma((NY,)),
            dma((STEPS,)), dma((STEPS,)), dma((2 * STEPS,)), dma((2 * STEPS,)), dma((2 * STEPS,)), dma((2 * STEPS,)),
            dma((STEPS,)), dma((STEPS,)),
            dma((2,)), dma, dma, dma, dma, dma, dma, dma,
        ]
        + [dma, dma((Ring.COUNT,)), dma, dma((Ring.COUNT,))] * 3
        + [dma, dma((6,)), dma, dma] * 2
        + [pltpu.SemaphoreType.REGULAR((2,))],
        compiler_params=pltpu.CompilerParams(
            collective_id=0, has_side_effects=True, vmem_limit_bytes=48 * 1024 * 1024
        ),
    )(*[pltpu.with_memory_space_constraint(x, pltpu.HBM) for x in (tokens, gain, w_up[0], w_down[0], cotangent[0])])
    return states[None], grad[None]


def solution(mesh):
    torus = Mesh(
        mesh.devices.reshape(mesh.shape["section"], NZ, NA, NY, NB), ("section", "z", "a", "y", "b")
    )
    dp, tensor = ("z", "a"), ("y", "b")
    in_specs = (
        P(dp, tensor),
        P("section", tensor),
        P("section", dp, tensor),
        P("section", tensor, dp),
        P("section", dp, None),
    )
    out_specs = (P("section", dp, tensor), P("section", tensor, dp))
    return jax.shard_map(body, mesh=torus, in_specs=in_specs, out_specs=out_specs, check_vma=False)
```
